128 devices in a mesh: depth: 4 (over z), col: 4 (over y), row: 8 (over x, core).
Axes of the slice: x: 4, y: 4, z: 4, core: 2. Of those that a mesh axis runs over, the one named last changes fastest.
Arguments:
- weight: bfloat16 [12288, 12288], P(('row', 'depth'), 'col')
- rhs_stack: bfloat16 [3, 12288, 8192], P(None, ('row', 'depth'), 'col')
Outputs:
- output: bfloat16 [3, 12288, 8192], P(None, ('row', 'depth'), 'col')
All inputs are finite; a program needn't handle non-finite values.
Results may differ from the reference program's by a relative error of at most 0.001.
Values are sent between devices in bfloat16 or wider.
A program may use at most 1 GiB of HBM per device.

```python
import jax
import jax.numpy as jnp
from jax import lax

N = 12288
RHS_COLS = 8192


def setup_inputs(seed: int = 0) -> dict:
    base_key = jax.random.key(seed)
    key_w, key_x = jax.random.split(base_key)
    weight = jax.random.normal(key_w, (N, N), jnp.float32) * (N ** -0.5) + 2.0 / N
    rhs_stack = jax.random.normal(key_x, (3, N, RHS_COLS), jnp.float32) + 0.5
    return {"weight": weight.astype(jnp.bfloat16), "rhs_stack": rhs_stack.astype(jnp.bfloat16)}


def reference(weight, rhs_stack):
    def one_product(rhs_block):
        return jnp.dot(weight, rhs_block, preferred_element_type=jnp.float32).astype(jnp.bfloat16)
    return lax.map(one_product, rhs_stack)
```

```python
import functools

import jax
import jax.numpy as jnp
from jax import lax
from jax.experimental import pallas as pl
from jax.experimental.pallas import tpu as pltpu
from jax.sharding import PartitionSpec as P

MESH = pl.DeviceIdType.MESH
MODES = "babababbabab"
A_PIECES = 4
SLOTS = 3
DEPTH_Q = 2
RATE = {"xp": 46.0e3, "xm": 46.0e3, "yp": 46.0e3, "ym": 46.0e3, "zl": 46.0e3, "zh": 46.0e3, "dd": 250.0e3}
LAT = {"dd": 1.5}


def make_plan(chunks, modes, unit, a_unit, half_us):
    sends = {}

    def add(name, link, size, deps, key):
        sends[name] = (link, size, frozenset(deps), key)

    need = {}
    for j in range(chunks):
        S, L = ("S", j), ("L", j)
        add(L, "zl", unit, [], j - 1)
        if modes[j] == "b":
            add(("H", j), "zh", 2 * unit, [S, L], j - 1.5)
            add(("R1", j), "xp", 4 * unit, [S, L, ("H", j)], (j, 1))
            add(("L1", j), "xm", 4 * unit, [S, L, ("H", j)], (j, 1))
            add(("R2", j), "xp", 2 * unit, [("R1", j)], (j, 0))
            add(("L2", j), "xm", 2 * unit, [("L1", j)], (j, 0))
            got = {0: [S, L, ("H", j)], -1: [("R1", j)], 1: [("L1", j)], 2: [("R2", j), ("L2", j)]}
        else:
            add(("R1", j), "xp", 2 * unit, [S, L], (j, 1))
            add(("L1", j), "xm", 2 * unit, [S, L], (j, 1))
            add(("R2", j), "xp", unit, [("R1", j)], (j, 0))
            add(("L2", j), "xm", unit, [("L1", j)], (j, 0))
            pre = {0: [S, L], -1: [("R1", j)], 1: [("L1", j)], 2: [("R2", j), ("L2", j)]}
            got = {}
            for d in (0, -1, 1, 2):
                add(("H", j, d), "zh", 2 * unit, pre[d], j)
                got[d] = pre[d] + [("H", j, d)]
        for d in (0, -1, 1, 2):
            add(("D", j, d), "dd", 4 * unit, got[d], j)
            need[j, d] = got[d] + [("D", j, d)]
        add(("Y", j), "zl", unit, [("C", j)], j)
    a_need = [("AS",)]
    for q in range(A_PIECES):
        add(("AL", q), "zl", a_unit, [("AS",)], 0.75 * q)
        for t in (0, 1):
            dep = [("AS",)] if t == 0 else [("AL", q)]
            add(("AR1", t, q), "yp", a_unit, dep, 4 * t + q)
            add(("AL1", t, q), "ym", a_unit, dep, 4 * t + q)
            a_need += [("AR1", t, q), ("AL1", t, q)]
        add(("AR2", q), "yp", a_unit, [("AR1", 0, q)], 8 + q)
        add(("AL2", q), "ym", a_unit, [("AL1", 1, q)], 8 + q)
        a_need += [("AL", q), ("AR2", q), ("AL2", q)]

    tasks = []
    for j in range(chunks):
        if j < chunks - 1:
            tasks += [(j, (0, -1)), (j, (1, 2))]
        else:
            tasks += [(j, (0,)), (j, (-1,)), (j, (1,)), (j, (2,))]

    prog = []
    t = 0.0
    at = {("AS",): 3.0}
    for j in range(chunks):
        at[("S", j)] = 2.5 + 0.3 * j
    done = set()
    waiting = dict(sends)
    busy = {k: 0.0 for k in RATE}
    out = {k: [] for k in RATE}
    loads = computed = 0
    while True:
        for link in RATE:
            out[link] = [e for e in out[link] if e > t]
            while len(out[link]) < DEPTH_Q:
                ready = [n for n, s in waiting.items() if s[0] == link and s[2] <= done]
                if not ready:
                    break
                name = min(ready, key=lambda n: (waiting[n][3], str(n)))
                size = waiting.pop(name)[1]
                busy[link] = max(busy[link], t + 0.2) + size / RATE[link]
                out[link].append(busy[link])
                at[name] = busy[link] + LAT.get(link, 2.0)
                prog.append(("start", name))
        if loads < len(tasks) and loads - computed < SLOTS:
            j, ds = tasks[loads]
            if all(set(need[j, d]) <= done for d in ds):
                prog.append(("load", loads))
                at["ld", loads] = t + 1.0 + 0.5 * len(ds)
                loads += 1
                continue
        now = sorted((v, str(n), n) for n, v in at.items() if n not in done and v <= t)
        if now:
            name = now[0][2]
            done.add(name)
            prog.append(("wait", name))
            continue
        if computed < loads and ("ld", computed) in done and set(a_need) <= done:
            prog.append(("compute", computed))
            j, ds = tasks[computed]
            t += 0.5 * half_us * len(ds)
            computed += 1
            if computed == len(tasks) or tasks[computed][0] != j:
                at["C", j] = t
                done.add(("C", j))
            continue
        later = [v for n, v in at.items() if n not in done]
        later += [e for link in RATE for e in out[link] if e > t]
        if not later:
            break
        t = min(later)
    if waiting or computed < len(tasks):
        raise ValueError("plan stuck")
    return prog, tasks, list(sends), t


def body(prog, tasks, names, modes, dims, a_ref, x_ref, y_ref, xg, av, xv, xs, yv, acc, ssem, rsem, lsem, osem, vsem):
    chunks, per_r, s, kb, width, kk = dims
    z, y, i = lax.axis_index("depth"), lax.axis_index("col"), lax.axis_index("row")
    x, c = i // 2, i % 2
    zh, pi = z // 2, z % 2
    nu = (zh + pi) % 2
    zl_peer = 2 * zh + 1 - pi
    zh_peer = 3 - z
    half = per_r * width

    def xat(d):
        return (x + d + 4) % 4

    def yat(d):
        return (y + d + 4) % 4

    dev = {
        "xp": (z, y, 2 * xat(1) + c),
        "xm": (z, y, 2 * xat(-1) + c),
        "yp": (z, yat(1), i),
        "ym": (z, yat(-1), i),
        "zl": (zl_peer, y, i),
        "zh": (zh_peer, y, i),
        "dd": (z, y, 2 * x + 1 - c),
    }

    def cols(j, part):
        return pl.ds(pl.multiple_of(part * half + (j % per_r) * width, 128), width)

    rows_a = s // A_PIECES

    def arow(which, q):
        return pl.ds(pl.multiple_of(which * s + q * rows_a, 16), rows_a)

    def krow(core, first, count):
        return pl.ds(pl.multiple_of((4 * core + first) * s, 16), count * s)

    def yrow(which):
        return pl.ds(pl.multiple_of(which * s, 16), s)

    def ends(name, recv):
        kind = name[0]
        if kind in ("AL", "AR1", "AL1", "AR2", "AL2"):
            q = name[-1]
            if kind == "AL":
                who = 1 - pi if recv else pi
                ref = av.at[y, arow(who, q)]
                return ref, ref, "zl"
            right = kind in ("AR1", "AR2")
            step = (-1 if right else 1) if recv else 0
            if kind in ("AR1", "AL1"):
                who = pi if name[1] == 0 else 1 - pi
                ref = av.at[yat(step), arow(who, q)]
            else:
                who = pi if right else 1 - pi
                ref = av.at[yat(step + (-1 if right else 1)), arow(who, q)]
            return ref, ref, "yp" if right else "ym"
        j = name[1]
        r = j // per_r
        if kind == "L":
            ref = xg.at[j, x, krow(c, zl_peer if recv else z, 1)]
            return (ref if recv else x_ref.at[r, :, cols(j, 1 - nu)]), ref, "zl"
        if kind == "Y":
            part = 1 - nu if recv else nu
            ref = y_ref.at[r, :, cols(j, part)]
            return yv.at[j, yrow(1 - pi)], ref, "zl"
        if kind == "D":
            ref = xg.at[j, xat(name[2]), krow(1 - c if recv else c, 0, 4)]
            return ref, ref, "dd"
        mine = krow(c, 2 * zh, 2)
        if kind == "H":
            d = name[2] if len(name) > 2 else 0
            ref = xg.at[j, xat(d), krow(c, 2 * (1 - zh), 2) if recv else mine]
            return ref, ref, "zh"
        right = kind[0] == "R"
        step = (-1 if right else 1) if recv else 0
        if modes[j] == "b":
            first = krow(c, 0, 4)
            second = krow(c, 0 if right else 2, 2)
        else:
            first = mine
            second = krow(c, 2 * zh if right else 2 * zh + 1, 1)
        if kind[1] == "1":
            ref = xg.at[j, xat(step), first]
        else:
            ref = xg.at[j, xat(step + (-1 if right else 1)), second]
        return ref, ref, "xp" if right else "xm"

    index = {n: k for k, n in enumerate(names)}

    def remote(name, recv=False):
        src, dst, link = ends(name, recv)
        return pltpu.make_async_remote_copy(
            src_ref=src, dst_ref=dst, send_sem=ssem.at[index[name]], recv_sem=rsem.at[index[name]],
            device_id=dev[link], device_id_type=MESH)

    def stage_in(j):
        return pltpu.make_async_copy(x_ref.at[j // per_r, :, cols(j, nu)], xs.at[j], lsem.at[j])

    def stage_out(j):
        return pltpu.make_async_copy(xs.at[j], xg.at[j, x, krow(c, z, 1)], lsem.at[chunks + j])

    def a_in():
        return pltpu.make_async_copy(a_ref, av.at[y, yrow(pi)], lsem.at[2 * chunks])

    def y_out(j):
        return pltpu.make_async_copy(yv.at[j, yrow(pi)], y_ref.at[j // per_r, :, cols(j, nu)], osem.at[j])

    def load(task, b):
        j, ds = tasks[task]
        slot = task % SLOTS
        return pltpu.make_async_copy(xg.at[j, xat(ds[b])], xv.at[slot, b], vsem.at[2 * slot + b])

    barrier = pltpu.get_barrier_semaphore()
    for peer in dev.values():
        pl.semaphore_signal(barrier, inc=1, device_id=peer, device_id_type=MESH)
    for j in range(chunks):
        stage_in(j).start()
    a_in().start()
    pl.semaphore_wait(barrier, len(dev))

    staged = [False]

    def finish_stage():
        for j in range(chunks):
            stage_in(j).wait()
            stage_out(j).start()
        staged[0] = True

    received = set()
    for op, what in prog:
        if op == "start":
            remote(what).start()
        elif op == "load":
            for b in range(len(tasks[what][1])):
                load(what, b).start()
        elif op == "wait":
            if not staged[0]:
                finish_stage()
            if what[0] == "S":
                stage_out(what[1]).wait()
            elif what[0] == "AS":
                a_in().wait()
            elif what[0] == "ld":
                for b in range(len(tasks[what[1]][1])):
                    load(what[1], b).wait()
            elif what[0] != "C":
                remote(what, True).wait_recv()
                received.add(what)
        else:
            j, ds = tasks[what]
            slot = what % SLOTS
            if what == 0 or tasks[what - 1][0] != j:
                acc[...] = jnp.zeros_like(acc)
            per = kb // kk
            base = ds[0]
            stride = ds[1] - ds[0] if len(ds) > 1 else 0

            def step(n, carry, slot=slot, base=base, stride=stride):
                b, k = n // per, n % per
                block = (x + base + 4 + stride * b) % 4
                lanes = pl.ds(pl.multiple_of(k * kk, 128), kk)
                acc[...] += jnp.dot(av[block, :, lanes], xv[slot, b, lanes, :], preferred_element_type=jnp.float32)
                return carry

            lax.fori_loop(0, per * len(ds), step, 0)
            if what + 1 == len(tasks) or tasks[what + 1][0] != j:
                yv[j] = acc[...].astype(yv.dtype)
                y_out(j).start()

    for name in names:
        if name not in received:
            remote(name, True).wait_recv()
    for name in names:
        remote(name).wait_send()
    for j in range(chunks):
        y_out(j).wait()


def solution(mesh):
    def local(a, x):
        rhs, s, xc = x.shape
        kb = a.shape[1]
        width = 256 if xc % 512 == 0 else xc // 2
        per_r = xc // 2 // width
        chunks = rhs * per_r
        modes = (MODES * chunks)[:chunks]
        kk = 1024 if kb % 1024 == 0 else 256
        prog, tasks, names, _ = make_plan(chunks, modes, 2 * s * width, 2 * s * kb // A_PIECES, 2.9)
        dims = (chunks, per_r, s, kb, width, kk)
        any_spec = pl.BlockSpec(memory_space=pl.ANY)
        y, _ = pl.pallas_call(
            functools.partial(body, prog, tasks, names, modes, dims),
            out_shape=(jax.ShapeDtypeStruct(x.shape, x.dtype), jax.ShapeDtypeStruct((chunks, 4, kb, width), x.dtype)),
            in_specs=[any_spec, any_spec],
            out_specs=(any_spec, any_spec),
            scratch_shapes=[
                pltpu.VMEM((4, 2 * s, kb), a.dtype),
                pltpu.VMEM((SLOTS, 2, kb, width), x.dtype),
                pltpu.VMEM((chunks, s, width), x.dtype),
                pltpu.VMEM((chunks, 2 * s, width), x.dtype),
                pltpu.VMEM((2 * s, width), jnp.float32),
                pltpu.SemaphoreType.DMA((len(names),)),
                pltpu.SemaphoreType.DMA((len(names),)),
                pltpu.SemaphoreType.DMA((2 * chunks + 1,)),
                pltpu.SemaphoreType.DMA((chunks,)),
                pltpu.SemaphoreType.DMA((2 * SLOTS,)),
            ],
            compiler_params=pltpu.CompilerParams(collective_id=0, has_side_effects=True, vmem_limit_bytes=60 * 1024 * 1024),
        )(a, x)
        return y

    spec_a = P(("row", "depth"), "col")
    spec_x = P(None, ("row", "depth"), "col")
    return jax.shard_map(local, mesh=mesh, in_specs=(spec_a, spec_x), out_specs=spec_x, check_vma=False)
```

```python
import functools

import jax
import jax.numpy as jnp
from jax import lax
from jax.experimental import pallas as pl
from jax.experimental.pallas import tpu as pltpu
from jax.sharding import PartitionSpec as P

MESH = pl.DeviceIdType.MESH
MODES = "abbabbaabbabb"
A_PIECES = 4
SLOTS = 3
DEPTH_Q = 2
RATE = {"xp": 46.0e3, "xm": 46.0e3, "yp": 46.0e3, "ym": 46.0e3, "zl": 46.0e3, "zh": 46.0e3, "dd": 250.0e3}
LAT = {"dd": 1.5}


def make_plan(units, modes, a_unit, half_us):
    sends = {}
    chunks = len(units)

    def add(name, link, size, deps, key):
        sends[name] = (link, size, frozenset(deps), key)

    need = {}
    for j in range(chunks):
        S, L, unit = ("S", j), ("L", j), units[j]
        add(L, "zl", unit, [], j - 1)
        if modes[j] == "b":
            add(("H", j, 0), "zh", unit, [], j - 1.5)
            add(("H", j, 1), "zh", unit, [L], j - 1.5)
            h = [("H", j, 0), ("H", j, 1)]
            for way, link in (("R", "xp"), ("L", "xm")):
                add((way + "1", j, 0), link, 2 * unit, [S, L], (j, 1))
                add((way + "1", j, 1), link, 2 * unit, h, (j, 1))
            add(("R2", j), "xp", 2 * unit, [("R1", j, 0)], (j, 0))
            add(("L2", j), "xm", 2 * unit, [("L1", j, 1)], (j, 0))
            got = {0: [S, L] + h, -1: [("R1", j, 0), ("R1", j, 1)], 1: [("L1", j, 0), ("L1", j, 1)], 2: [("R2", j), ("L2", j)]}
        else:
            for way, link in (("R", "xp"), ("L", "xm")):
                add((way + "1", j, 0), link, unit, [], (j, 1))
                add((way + "1", j, 1), link, unit, [L], (j, 1))
            add(("R2", j), "xp", unit, [("R1", j, 0)], (j, 0))
            add(("L2", j), "xm", unit, [("L1", j, 1)], (j, 0))
            pre = {0: [S, L], -1: [("R1", j, 0), ("R1", j, 1)], 1: [("L1", j, 0), ("L1", j, 1)], 2: [("R2", j), ("L2", j)]}
            got = {}
            for d in (0, -1, 1, 2):
                add(("H", j, d), "zh", 2 * unit, pre[d], j)
                got[d] = pre[d] + [("H", j, d)]
        for d in (0, -1, 1, 2):
            add(("D", j, d), "dd", 4 * unit, got[d], j)
            need[j, d] = got[d] + [("D", j, d)]
        add(("Y", j), "zl", unit, [("C", j)], j)
    a_need = [("AS",)]
    for q in range(A_PIECES):
        add(("AL", q), "zl", a_unit, [("AS",)], 0.75 * q)
        for t in (0, 1):
            dep = [("AS",)] if t == 0 else [("AL", q)]
            add(("AR1", t, q), "yp", a_unit, dep, 4 * t + q)
            add(("AL1", t, q), "ym", a_unit, dep, 4 * t + q)
            a_need += [("AR1", t, q), ("AL1", t, q)]
        add(("AR2", q), "yp", a_unit, [("AR1", 0, q)], 8 + q)
        add(("AL2", q), "ym", a_unit, [("AL1", 1, q)], 8 + q)
        a_need += [("AL", q), ("AR2", q), ("AL2", q)]

    tasks = []
    for j in range(chunks):
        if j < chunks - 1:
            tasks += [(j, (0, -1)), (j, (1, 2))]
        else:
            tasks += [(j, (0,)), (j, (-1,)), (j, (1,)), (j, (2,))]

    prog = []
    t = 0.0
    at = {("AS",): 3.0}
    for j in range(chunks):
        at[("S", j)] = 2.5 + 0.3 * j
    done = set()
    waiting = dict(sends)
    busy = {k: 0.0 for k in RATE}
    out = {k: [] for k in RATE}
    loads = computed = 0
    while True:
        for link in RATE:
            out[link] = [e for e in out[link] if e > t]
            while len(out[link]) < DEPTH_Q:
                ready = [n for n, s in waiting.items() if s[0] == link and s[2] <= done]
                if not ready:
                    break
                name = min(ready, key=lambda n: (waiting[n][3], str(n)))
                size = waiting.pop(name)[1]
                busy[link] = max(busy[link], t + 0.2) + size / RATE[link]
                out[link].append(busy[link])
                at[name] = busy[link] + LAT.get(link, 2.0)
                prog.append(("start", name))
        if loads < len(tasks) and loads - computed < SLOTS:
            j, ds = tasks[loads]
            if all(set(need[j, d]) <= done for d in ds):
                prog.append(("load", loads))
                at["ld", loads] = t + 1.0 + 0.5 * len(ds)
                loads += 1
                continue
        now = sorted((v, str(n), n) for n, v in at.items() if n not in done and v <= t)
        if now:
            name = now[0][2]
            done.add(name)
            prog.append(("wait", name))
            continue
        if computed < loads and ("ld", computed) in done and set(a_need) <= done:
            prog.append(("compute", computed))
            j, ds = tasks[computed]
            t += 0.5 * half_us * len(ds)
            computed += 1
            if computed == len(tasks) or tasks[computed][0] != j:
                at["C", j] = t
                done.add(("C", j))
            continue
        later = [v for n, v in at.items() if n not in done]
        later += [e for link in RATE for e in out[link] if e > t]
        if not later:
            break
        t = min(later)
    if waiting or computed < len(tasks):
        raise ValueError("plan stuck")
    return prog, tasks, list(sends), t


def body(prog, tasks, names, modes, dims, a_ref, x_ref, y_ref, xg, av, xv, xs, yv, acc, ssem, rsem, lsem, osem, vsem):
    layout, s, kb, half, kk = dims
    chunks = len(layout)
    z, y, i = lax.axis_index("depth"), lax.axis_index("col"), lax.axis_index("row")
    x, c = i // 2, i % 2
    zh, pi = z // 2, z % 2
    nu = (zh + pi) % 2
    zl_peer = 2 * zh + 1 - pi
    zh_peer = 3 - z

    def xat(d):
        return (x + d + 4) % 4

    def yat(d):
        return (y + d + 4) % 4

    dev = {
        "xp": (z, y, 2 * xat(1) + c),
        "xm": (z, y, 2 * xat(-1) + c),
        "yp": (z, yat(1), i),
        "ym": (z, yat(-1), i),
        "zl": (zl_peer, y, i),
        "zh": (zh_peer, y, i),
        "dd": (z, y, 2 * x + 1 - c),
    }

    def cols(j, part):
        return pl.ds(pl.multiple_of(part * half + layout[j][1], 128), layout[j][2])

    def lane(j):
        return pl.ds(0, layout[j][2])

    def xin(j, part):
        return x_ref.at[layout[j][0], :, cols(j, part)]

    def xgat(j, block, rows):
        return xg.at[j, block, rows, lane(j)]

    rows_a = s // A_PIECES

    def arow(which, q):
        return pl.ds(pl.multiple_of(which * s + q * rows_a, 16), rows_a)

    def krow(core, first, count):
        return pl.ds(pl.multiple_of((4 * core + first) * s, 16), count * s)

    def yrow(which):
        return pl.ds(pl.multiple_of(which * s, 16), s)

    def ends(name, recv):
        kind = name[0]
        if kind in ("AL", "AR1", "AL1", "AR2", "AL2"):
            q = name[-1]
            if kind == "AL":
                who = 1 - pi if recv else pi
                ref = av.at[y, arow(who, q)]
                return ref, ref, "zl"
            right = kind in ("AR1", "AR2")
            step = (-1 if right else 1) if recv else 0
            if kind in ("AR1", "AL1"):
                who = pi if name[1] == 0 else 1 - pi
                ref = av.at[yat(step), arow(who, q)]
            else:
                who = pi if right else 1 - pi
                ref = av.at[yat(step + (-1 if right else 1)), arow(who, q)]
            return ref, ref, "yp" if right else "ym"
        j = name[1]
        if kind == "L":
            ref = xgat(j, x, krow(c, zl_peer if recv else z, 1))
            return (ref if recv else xin(j, 1 - nu)), ref, "zl"
        if kind == "Y":
            part = 1 - nu if recv else nu
            ref = y_ref.at[layout[j][0], :, cols(j, part)]
            return yv.at[j, yrow(1 - pi), lane(j)], ref, "zl"
        if kind == "D":
            ref = xgat(j, xat(name[2]), krow(1 - c if recv else c, 0, 4))
            return ref, ref, "dd"
        own, pair, other = krow(c, z, 1), krow(c, 2 * zh, 2), krow(c, 2 * (1 - zh), 2)
        if kind == "H":
            if modes[j] == "b":
                at = z if name[2] == 0 else zl_peer
                ref = xgat(j, x, krow(c, 3 - at if recv else at, 1))
                return (xin(j, nu) if name[2] == 0 and not recv else ref), ref, "zh"
            ref = xgat(j, xat(name[2]), other if recv else pair)
            return ref, ref, "zh"
        right = kind[0] == "R"
        link = "xp" if right else "xm"
        step = (-1 if right else 1) if recv else 0
        if modes[j] == "b":
            parts = (pair, other)
        else:
            parts = (own, krow(c, zl_peer, 1))
        if kind[1] == "1":
            ref = xgat(j, xat(step), parts[name[2]])
            direct = modes[j] == "a" and name[2] == 0 and not recv
            return (xin(j, nu) if direct else ref), ref, link
        ref = xgat(j, xat(step + (-1 if right else 1)), parts[0 if right else 1])
        return ref, ref, link

    index = {n: k for k, n in enumerate(names)}

    def remote(name, recv=False):
        src, dst, link = ends(name, recv)
        return pltpu.make_async_remote_copy(
            src_ref=src, dst_ref=dst, send_sem=ssem.at[index[name]], recv_sem=rsem.at[index[name]],
            device_id=dev[link], device_id_type=MESH)

    def stage_in(j):
        return pltpu.make_async_copy(xin(j, nu), xs.at[j, :, lane(j)], lsem.at[j])

    def stage_out(j):
        return pltpu.make_async_copy(xs.at[j, :, lane(j)], xgat(j, x, krow(c, z, 1)), lsem.at[chunks + j])

    def a_in():
        return pltpu.make_async_copy(a_ref, av.at[y, yrow(pi)], lsem.at[2 * chunks])

    def y_out(j):
        return pltpu.make_async_copy(yv.at[j, yrow(pi), lane(j)], y_ref.at[layout[j][0], :, cols(j, nu)], osem.at[j])

    def load(task, b):
        j, ds = tasks[task]
        slot = task % SLOTS
        return pltpu.make_async_copy(xgat(j, xat(ds[b]), pl.ds(0, kb)), xv.at[slot, b, :, lane(j)], vsem.at[2 * slot + b])

    barrier = pltpu.get_barrier_semaphore()
    for peer in dev.values():
        pl.semaphore_signal(barrier, inc=1, device_id=peer, device_id_type=MESH)
    for j in range(chunks):
        stage_in(j).start()
    a_in().start()
    pl.semaphore_wait(barrier, len(dev))

    staged = [False]

    def finish_stage():
        for j in range(chunks):
            stage_in(j).wait()
            stage_out(j).start()
        staged[0] = True

    received = set()
    for op, what in prog:
        if op == "start":
            remote(what).start()
        elif op == "load":
            for b in range(len(tasks[what][1])):
                load(what, b).start()
        elif op == "wait":
            if not staged[0]:
                finish_stage()
            if what[0] == "S":
                stage_out(what[1]).wait()
            elif what[0] == "AS":
                a_in().wait()
            elif what[0] == "ld":
                for b in range(len(tasks[what[1]][1])):
                    load(what[1], b).wait()
            elif what[0] != "C":
                remote(what, True).wait_recv()
                received.add(what)
        else:
            j, ds = tasks[what]
            slot = what % SLOTS
            if what == 0 or tasks[what - 1][0] != j:
                acc[:, lane(j)] = jnp.zeros((2 * s, layout[j][2]), jnp.float32)
            per = kb // kk
            base = ds[0]
            stride = ds[1] - ds[0] if len(ds) > 1 else 0

            def step(n, carry, slot=slot, base=base, stride=stride, wide=lane(j)):
                b, k = n // per, n % per
                block = (x + base + 4 + stride * b) % 4
                lanes = pl.ds(pl.multiple_of(k * kk, 128), kk)
                acc[:, wide] += jnp.dot(av[block, :, lanes], xv[slot, b, lanes, wide], preferred_element_type=jnp.float32)
                return carry

            lax.fori_loop(0, per * len(ds), step, 0)
            if what + 1 == len(tasks) or tasks[what + 1][0] != j:
                yv[j, :, lane(j)] = acc[:, lane(j)].astype(yv.dtype)
                y_out(j).start()

    for name in names:
        if name not in received:
            remote(name, True).wait_recv()
    for name in names:
        remote(name).wait_send()
    for j in range(chunks):
        y_out(j).wait()


def solution(mesh):
    def local(a, x):
        rhs, s, xc = x.shape
        kb = a.shape[1]
        half = xc // 2
        width = 256 if half % 256 == 0 else 128
        layout = [(r, at, width) for r in range(rhs) for at in range(0, half, width)]
        if width == 256:
            r, at, _ = layout.pop()
            layout += [(r, at, 128), (r, at + 128, 128)]
        chunks = len(layout)
        modes = (MODES * chunks)[:chunks]
        kk = 1024 if kb % 1024 == 0 else 256
        units = [2 * s * w for _, _, w in layout]
        prog, tasks, names, _ = make_plan(units, modes, 2 * s * kb // A_PIECES, 2.9)
        dims = (layout, s, kb, half, kk)
        any_spec = pl.BlockSpec(memory_space=pl.ANY)
        y, _ = pl.pallas_call(
            functools.partial(body, prog, tasks, names, modes, dims),
            out_shape=(jax.ShapeDtypeStruct(x.shape, x.dtype), jax.ShapeDtypeStruct((chunks, 4, kb, width), x.dtype)),
            in_specs=[any_spec, any_spec],
            out_specs=(any_spec, any_spec),
            scratch_shapes=[
                pltpu.VMEM((4, 2 * s, kb), a.dtype),
                pltpu.VMEM((SLOTS, 2, kb, width), x.dtype),
                pltpu.VMEM((chunks, s, width), x.dtype),
                pltpu.VMEM((chunks, 2 * s, width), x.dtype),
                pltpu.VMEM((2 * s, width), jnp.float32),
                pltpu.SemaphoreType.DMA((len(names),)),
                pltpu.SemaphoreType.DMA((len(names),)),
                pltpu.SemaphoreType.DMA((2 * chunks + 1,)),
                pltpu.SemaphoreType.DMA((chunks,)),
                pltpu.SemaphoreType.DMA((2 * SLOTS,)),
            ],
            compiler_params=pltpu.CompilerParams(collective_id=0, has_side_effects=True, vmem_limit_bytes=60 * 1024 * 1024),
        )(a, x)
        return y

    spec_a = P(("row", "depth"), "col")
    spec_x = P(None, ("row", "depth"), "col")
    return jax.shard_map(local, mesh=mesh, in_specs=(spec_a, spec_x), out_specs=spec_x, check_vma=False)
```

```python
import functools

import jax
import jax.numpy as jnp
from jax import lax
from jax.experimental import pallas as pl
from jax.experimental.pallas import tpu as pltpu
from jax.sharding import PartitionSpec as P

MESH = pl.DeviceIdType.MESH
MODES = "abbabbaabbabb"
A_PIECES = 4
SLOTS = 5
DEPTH_Q = 3
TAIL_CHUNKS = 2
MARGIN = 2.0
PLAN_LAT = 2.5
BLOCK_US = 1.8
RATE = {"xp": 46.0e3, "xm": 46.0e3, "yp": 46.0e3, "ym": 46.0e3, "zl": 46.0e3, "zh": 46.0e3, "dd": 200.0e3}
LAT = {"dd": 2.5}


def make_plan(units, modes, a_unit, block_us):
    sends = {}
    chunks = len(units)

    def add(name, link, size, deps, key):
        sends[name] = (link, size, frozenset(deps), key)

    need = {}
    for j in range(chunks):
        S, L, unit = ("S", j), ("L", j), units[j]
        add(L, "zl", unit, [], j - 1)
        if modes[j] == "b":
            add(("H", j, 0), "zh", unit, [], j - 1.5)
            add(("H", j, 1), "zh", unit, [L], j - 1.5)
            h = [("H", j, 0), ("H", j, 1)]
            for way, link in (("R", "xp"), ("L", "xm")):
                add((way + "1", j, 0), link, 2 * unit, [S, L], (j, 1))
                add((way + "1", j, 1), link, 2 * unit, h, (j, 1))
            add(("R2", j), "xp", 2 * unit, [("R1", j, 0)], (j, 0))
            add(("L2", j), "xm", 2 * unit, [("L1", j, 1)], (j, 0))
            got = {0: [S, L] + h, -1: [("R1", j, 0), ("R1", j, 1)], 1: [("L1", j, 0), ("L1", j, 1)], 2: [("R2", j), ("L2", j)]}
        else:
            for way, link in (("R", "xp"), ("L", "xm")):
                add((way + "1", j, 0), link, unit, [], (j, 1))
                add((way + "1", j, 1), link, unit, [L], (j, 1))
            add(("R2", j), "xp", unit, [("R1", j, 0)], (j, 0))
            add(("L2", j), "xm", unit, [("L1", j, 1)], (j, 0))
            pre = {0: [S, L], -1: [("R1", j, 0), ("R1", j, 1)], 1: [("L1", j, 0), ("L1", j, 1)], 2: [("R2", j), ("L2", j)]}
            got = {}
            for d in (0, -1, 1, 2):
                add(("H", j, d), "zh", 2 * unit, pre[d], j)
                got[d] = pre[d] + [("H", j, d)]
        for d in (0, -1, 1, 2):
            add(("D", j, d), "dd", 4 * unit, got[d], j)
            need[j, d] = got[d] + [("D", j, d)]
        add(("Y", j), "zl", unit, [("C", j)], j)
    a_need = {0: [("AS",)], 1: [], -1: [], 2: []}
    for q in range(A_PIECES):
        add(("AL", q), "zl", a_unit, [("AS",)], 0.75 * q)
        for t in (0, 1):
            dep = [("AS",)] if t == 0 else [("AL", q)]
            add(("AR1", t, q), "yp", a_unit, dep, 4 * t + q)
            add(("AL1", t, q), "ym", a_unit, dep, 4 * t + q)
            a_need[-1].append(("AR1", t, q))
            a_need[1].append(("AL1", t, q))
        add(("AR2", q), "yp", a_unit, [("AR1", 0, q)], 8 + q)
        add(("AL2", q), "ym", a_unit, [("AL1", 1, q)], 8 + q)
        a_need[0].append(("AL", q))
        a_need[2] += [("AR2", q), ("AL2", q)]
    a_all = sum(a_need.values(), [])

    tasks = []
    left = []
    for j in range(chunks):
        for e in (0, -1, 1, 2):
            if j < chunks - TAIL_CHUNKS:
                left.append((j, "y", e, sum((need[j, d] for d in (0, -1, 1, 2)), []), a_need[e]))
            else:
                left.append((j, "x", e, need[j, e], a_all))

    prog = []
    t = 0.0
    at = {("AS",): 3.0}
    for j in range(chunks):
        at[("S", j)] = 2.5 + 0.3 * j
    eager = set().union(*(v[2] for v in sends.values()))
    done = set()
    waiting = dict(sends)
    busy = {k: 0.0 for k in RATE}
    out = {k: [] for k in RATE}
    ready_at = {}
    computed = 0
    parts = {}

    def arrived(events, when):
        return all(n in done or at.get(n, 1e9) <= when for n in events)

    def settle(events):
        for n in events:
            if n not in done:
                done.add(n)
                prog.append(("wait", n))

    while True:
        for link in RATE:
            out[link] = [e for e in out[link] if e > t]
            while len(out[link]) < DEPTH_Q:
                ready = [n for n, v in waiting.items() if v[0] == link and v[2] <= done]
                if not ready:
                    break
                name = min(ready, key=lambda n: (waiting[n][3], str(n)))
                size = waiting.pop(name)[1]
                busy[link] = max(busy[link], t + 0.2) + size / RATE[link]
                out[link].append(busy[link])
                at[name] = busy[link] + LAT.get(link, PLAN_LAT)
                prog.append(("start", name))
        now = sorted((v, str(n), n) for n, v in at.items() if n in eager and n not in done and v <= t)
        if now:
            settle([now[0][2]])
            continue
        margin = MARGIN if len(left) > 4 * TAIL_CHUNKS else 0.0
        if len(tasks) - computed < SLOTS:
            pick = [v for v in left if arrived(v[3], t - margin) and arrived(v[4], t - margin)]
            if pick:
                task = pick[0]
                left.remove(task)
                settle(task[3])
                settle(task[4])
                prog.append(("load", len(tasks)))
                ready_at[len(tasks)] = t + 1.7
                tasks.append(task[:3])
                continue
        if computed < len(tasks) and ready_at[computed] <= t:
            prog.append(("compute", computed))
            j = tasks[computed][0]
            t += block_us
            computed += 1
            parts[j] = parts.get(j, 0) + 1
            if parts[j] == 4:
                done.add(("C", j))
            continue
        later = [v for n, v in at.items() if n in eager and n not in done]
        later += [e for link in RATE for e in out[link] if e > t]
        later += [v for k, v in ready_at.items() if k >= computed]
        later += [v + margin for n, v in at.items() if n not in done and v + margin > t]
        later = [v for v in later if v > t]
        if not later:
            break
        t = min(later)
    if waiting or left or computed < len(tasks):
        raise ValueError("plan stuck")
    return prog, tasks, list(sends), t


def body(prog, tasks, names, modes, dims, a_ref, x_ref, y_ref, xg, av, xv, xs, yv, acc, ssem, rsem, lsem, osem, vsem):
    layout, s, kb, half, kk = dims
    chunks = len(layout)
    z, y, i = lax.axis_index("depth"), lax.axis_index("col"), lax.axis_index("row")
    x, c = i // 2, i % 2
    zh, pi = z // 2, z % 2
    nu = (zh + pi) % 2
    zl_peer = 2 * zh + 1 - pi
    zh_peer = 3 - z

    def xat(d):
        return (x + d + 4) % 4

    def yat(d):
        return (y + d + 4) % 4

    dev = {
        "xp": (z, y, 2 * xat(1) + c),
        "xm": (z, y, 2 * xat(-1) + c),
        "yp": (z, yat(1), i),
        "ym": (z, yat(-1), i),
        "zl": (zl_peer, y, i),
        "zh": (zh_peer, y, i),
        "dd": (z, y, 2 * x + 1 - c),
    }

    def cols(j, part):
        return pl.ds(pl.multiple_of(part * half + layout[j][1], 128), layout[j][2])

    def lane(j):
        return pl.ds(0, layout[j][2])

    def xin(j, part):
        return x_ref.at[layout[j][0], :, cols(j, part)]

    def xgat(j, block, rows):
        return xg.at[j, block, rows, lane(j)]

    rows_a = s // A_PIECES

    def arow(which, q):
        return pl.ds(pl.multiple_of(which * s + q * rows_a, 16), rows_a)

    def krow(core, first, count):
        return pl.ds(pl.multiple_of((4 * core + first) * s, 16), count * s)

    def yrow(which):
        return pl.ds(pl.multiple_of(which * s, 16), s)

    def ends(name, recv):
        kind = name[0]
        if kind in ("AL", "AR1", "AL1", "AR2", "AL2"):
            q = name[-1]
            if kind == "AL":
                who = 1 - pi if recv else pi
                ref = av.at[y, arow(who, q)]
                return ref, ref, "zl"
            right = kind in ("AR1", "AR2")
            step = (-1 if right else 1) if recv else 0
            if kind in ("AR1", "AL1"):
                who = pi if name[1] == 0 else 1 - pi
                ref = av.at[yat(step), arow(who, q)]
            else:
                who = pi if right else 1 - pi
                ref = av.at[yat(step + (-1 if right else 1)), arow(who, q)]
            return ref, ref, "yp" if right else "ym"
        j = name[1]
        if kind == "L":
            ref = xgat(j, x, krow(c, zl_peer if recv else z, 1))
            return (ref if recv else xin(j, 1 - nu)), ref, "zl"
        if kind == "Y":
            part = 1 - nu if recv else nu
            ref = y_ref.at[layout[j][0], :, cols(j, part)]
            return yv.at[j, yrow(1 - pi), lane(j)], ref, "zl"
        if kind == "D":
            ref = xgat(j, xat(name[2]), krow(1 - c if recv else c, 0, 4))
            return ref, ref, "dd"
        own, pair, other = krow(c, z, 1), krow(c, 2 * zh, 2), krow(c, 2 * (1 - zh), 2)
        if kind == "H":
            if modes[j] == "b":
                at = z if name[2] == 0 else zl_peer
                ref = xgat(j, x, krow(c, 3 - at if recv else at, 1))
                return (xin(j, nu) if name[2] == 0 and not recv else ref), ref, "zh"
            ref = xgat(j, xat(name[2]), other if recv else pair)
            return ref, ref, "zh"
        right = kind[0] == "R"
        link = "xp" if right else "xm"
        step = (-1 if right else 1) if recv else 0
        if modes[j] == "b":
            parts = (pair, other)
        else:
            parts = (own, krow(c, zl_peer, 1))
        if kind[1] == "1":
            ref = xgat(j, xat(step), parts[name[2]])
            direct = modes[j] == "a" and name[2] == 0 and not recv
            return (xin(j, nu) if direct else ref), ref, link
        ref = xgat(j, xat(step + (-1 if right else 1)), parts[0 if right else 1])
        return ref, ref, link

    index = {n: k for k, n in enumerate(names)}

    def remote(name, recv=False):
        src, dst, link = ends(name, recv)
        return pltpu.make_async_remote_copy(
            src_ref=src, dst_ref=dst, send_sem=ssem.at[index[name]], recv_sem=rsem.at[index[name]],
            device_id=dev[link], device_id_type=MESH)

    def stage_in(j):
        return pltpu.make_async_copy(xin(j, nu), xs.at[j, :, lane(j)], lsem.at[j])

    def stage_out(j):
        return pltpu.make_async_copy(xs.at[j, :, lane(j)], xgat(j, x, krow(c, z, 1)), lsem.at[chunks + j])

    def a_in():
        return pltpu.make_async_copy(a_ref, av.at[y, yrow(pi)], lsem.at[2 * chunks])

    def y_out(j):
        return pltpu.make_async_copy(yv.at[j, yrow(pi), lane(j)], y_ref.at[layout[j][0], :, cols(j, nu)], osem.at[j])

    def load(task):
        j, axis, e = tasks[task]
        slot = task % SLOTS
        block = yat(e) if axis == "y" else xat(e)
        return pltpu.make_async_copy(xgat(j, block, pl.ds(0, kb)), xv.at[slot, :, lane(j)], vsem.at[slot])

    barrier = pltpu.get_barrier_semaphore()
    for peer in dev.values():
        pl.semaphore_signal(barrier, inc=1, device_id=peer, device_id_type=MESH)
    for j in range(chunks):
        stage_in(j).start()
    a_in().start()
    pl.semaphore_wait(barrier, len(dev))

    staged = [False]

    def finish_stage():
        for j in range(chunks):
            stage_in(j).wait()
            stage_out(j).start()
        staged[0] = True

    received = set()
    parts = [0] * chunks
    for op, what in prog:
        if op == "start":
            remote(what).start()
        elif op == "load":
            load(what).start()
        elif op == "wait":
            if not staged[0]:
                finish_stage()
            if what[0] == "S":
                stage_out(what[1]).wait()
            elif what[0] == "AS":
                a_in().wait()
            else:
                remote(what, True).wait_recv()
                received.add(what)
        else:
            j, axis, e = tasks[what]
            slot = what % SLOTS
            wide = lane(j)
            load(what).wait()
            if parts[j] == 0:
                acc[j, :, wide] = jnp.zeros((2 * s, layout[j][2]), jnp.float32)
            block = yat(e) if axis == "y" else xat(e)

            def step(k, carry, slot=slot, block=block, j=j, wide=wide):
                lanes = pl.ds(pl.multiple_of(k * kk, 128), kk)
                acc[j, :, wide] += jnp.dot(av[block, :, lanes], xv[slot, lanes, wide], preferred_element_type=jnp.float32)
                return carry

            lax.fori_loop(0, kb // kk, step, 0)
            parts[j] += 1
            if parts[j] == 4:
                yv[j, :, wide] = acc[j, :, wide].astype(yv.dtype)
                y_out(j).start()

    for name in names:
        if name not in received:
            remote(name, True).wait_recv()
    for name in names:
        remote(name).wait_send()
    for j in range(chunks):
        y_out(j).wait()


def solution(mesh):
    def local(a, x):
        rhs, s, xc = x.shape
        kb = a.shape[1]
        half = xc // 2
        width = 256 if half % 256 == 0 else 128
        layout = [(r, at, width) for r in range(rhs) for at in range(0, half, width)]
        if width == 256:
            r, at, _ = layout.pop()
            layout += [(r, at, 128), (r, at + 128, 128)]
        chunks = len(layout)
        modes = (MODES * chunks)[:chunks]
        kk = 1024 if kb % 1024 == 0 else 256
        units = [2 * s * w for _, _, w in layout]
        prog, tasks, names, _ = make_plan(units, modes, 2 * s * kb // A_PIECES, BLOCK_US)
        dims = (layout, s, kb, half, kk)
        any_spec = pl.BlockSpec(memory_space=pl.ANY)
        y, _ = pl.pallas_call(
            functools.partial(body, prog, tasks, names, modes, dims),
            out_shape=(jax.ShapeDtypeStruct(x.shape, x.dtype), jax.ShapeDtypeStruct((chunks, 4, kb, width), x.dtype)),
            in_specs=[any_spec, any_spec],
            out_specs=(any_spec, any_spec),
            scratch_shapes=[
                pltpu.VMEM((4, 2 * s, kb), a.dtype),
                pltpu.VMEM((SLOTS, kb, width), x.dtype),
                pltpu.VMEM((chunks, s, width), x.dtype),
                pltpu.VMEM((chunks, 2 * s, width), x.dtype),
                pltpu.VMEM((chunks, 2 * s, width), jnp.float32),
                pltpu.SemaphoreType.DMA((len(names),)),
                pltpu.SemaphoreType.DMA((len(names),)),
                pltpu.SemaphoreType.DMA((2 * chunks + 1,)),
                pltpu.SemaphoreType.DMA((chunks,)),
                pltpu.SemaphoreType.DMA((SLOTS,)),
            ],
            compiler_params=pltpu.CompilerParams(collective_id=0, has_side_effects=True, vmem_limit_bytes=60 * 1024 * 1024),
        )(a, x)
        return y

    spec_a = P(("row", "depth"), "col")
    spec_x = P(None, ("row", "depth"), "col")
    return jax.shard_map(local, mesh=mesh, in_specs=(spec_a, spec_x), out_specs=spec_x, check_vma=False)
```

```python
import functools

import jax
import jax.numpy as jnp
from jax import lax
from jax.experimental import pallas as pl
from jax.experimental.pallas import tpu as pltpu
from jax.sharding import PartitionSpec as P

MESH = pl.DeviceIdType.MESH
MODES = "abbabbaabbabb"
A_PIECES = 4
SLOTS = 5
DEPTH_Q = 3
TAIL_CHUNKS = 2
MARGIN = 2.0
PLAN_LAT = 2.5
BLOCK_US = 1.8
RATE = {"xp": 46.0e3, "xm": 46.0e3, "yp": 46.0e3, "ym": 46.0e3, "zl": 46.0e3, "zh": 46.0e3, "dd": 200.0e3}
LAT = {"dd": 2.5}


def make_plan(units, modes, a_unit, block_us):
    sends = {}
    chunks = len(units)

    def add(name, link, size, deps, key):
        sends[name] = (link, size, frozenset(deps), key)

    need = {}
    for j in range(chunks):
        S, L, unit = ("S", j), ("L", j), units[j]
        add(L, "zl", unit, [], j - 1)
        if modes[j] == "b":
            add(("H", j, 0), "zh", unit, [], j - 1.5)
            add(("H", j, 1), "zh", unit, [L], j - 1.5)
            h = [("H", j, 0), ("H", j, 1)]
            for way, link in (("R", "xp"), ("L", "xm")):
                add((way + "1", j, 0), link, 2 * unit, [S, L], (j, 1))
                add((way + "1", j, 1), link, 2 * unit, h, (j, 1))
            add(("R2", j), "xp", 2 * unit, [("R1", j, 0)], (j, 0))
            add(("L2", j), "xm", 2 * unit, [("L1", j, 1)], (j, 0))
            got = {0: [S, L] + h, -1: [("R1", j, 0), ("R1", j, 1)], 1: [("L1", j, 0), ("L1", j, 1)], 2: [("R2", j), ("L2", j)]}
        else:
            for way, link in (("R", "xp"), ("L", "xm")):
                add((way + "1", j, 0), link, unit, [], (j, 1))
                add((way + "1", j, 1), link, unit, [L], (j, 1))
            add(("R2", j), "xp", unit, [("R1", j, 0)], (j, 0))
            add(("L2", j), "xm", unit, [("L1", j, 1)], (j, 0))
            pre = {0: [S, L], -1: [("R1", j, 0), ("R1", j, 1)], 1: [("L1", j, 0), ("L1", j, 1)], 2: [("R2", j), ("L2", j)]}
            got = {}
            for d in (0, -1, 1, 2):
                add(("H", j, d), "zh", 2 * unit, pre[d], j)
                got[d] = pre[d] + [("H", j, d)]
        for d in (0, -1, 1, 2):
            add(("D", j, d), "dd", 4 * unit, got[d], j)
            need[j, d] = got[d] + [("D", j, d)]
        add(("Y", j), "zl", unit, [("C", j)], j)
    a_need = {0: [("AS",)], 1: [], -1: [], 2: []}
    for q in range(A_PIECES):
        add(("AL", q), "zl", a_unit, [("AS",)], 0.75 * q)
        for t in (0, 1):
            dep = [("AS",)] if t == 0 else [("AL", q)]
            add(("AR1", t, q), "yp", a_unit, dep, 4 * t + q)
            add(("AL1", t, q), "ym", a_unit, dep, 4 * t + q)
            a_need[-1].append(("AR1", t, q))
            a_need[1].append(("AL1", t, q))
        add(("AR2", q), "yp", a_unit, [("AR1", 0, q)], 8 + q)
        add(("AL2", q), "ym", a_unit, [("AL1", 1, q)], 8 + q)
        a_need[0].append(("AL", q))
        a_need[2] += [("AR2", q), ("AL2", q)]
    a_all = sum(a_need.values(), [])

    tasks = []
    left = []
    for j in range(chunks):
        for e in (0, -1, 1, 2):
            if j < chunks - TAIL_CHUNKS:
                left.append((j, "y", e, sum((need[j, d] for d in (0, -1, 1, 2)), []), a_need[e]))
            else:
                left.append((j, "x", e, need[j, e], a_all))

    prog = []
    t = 0.0
    at = {("AS",): 3.0}
    for j in range(chunks):
        at[("S", j)] = 2.5 + 0.3 * j
    eager = set().union(*(v[2] for v in sends.values()))
    done = set()
    waiting = dict(sends)
    busy = {k: 0.0 for k in RATE}
    out = {k: [] for k in RATE}
    ready_at = {}
    computed = 0
    parts = {}

    def arrived(events, when):
        return all(n in done or at.get(n, 1e9) <= when for n in events)

    def settle(events):
        for n in events:
            if n not in done:
                done.add(n)
                prog.append(("wait", n))

    while True:
        for link in RATE:
            out[link] = [e for e in out[link] if e > t]
            while len(out[link]) < DEPTH_Q:
                ready = [n for n, v in waiting.items() if v[0] == link and v[2] <= done]
                if not ready:
                    break
                name = min(ready, key=lambda n: (waiting[n][3], str(n)))
                size = waiting.pop(name)[1]
                busy[link] = max(busy[link], t + 0.2) + size / RATE[link]
                out[link].append(busy[link])
                at[name] = busy[link] + LAT.get(link, PLAN_LAT)
                prog.append(("start", name))
        now = sorted((v, str(n), n) for n, v in at.items() if n in eager and n not in done and v <= t)
        if now:
            settle([now[0][2]])
            continue
        margin = MARGIN if len(left) > 4 * TAIL_CHUNKS else 0.0
        if len(tasks) - computed < SLOTS:
            pick = [v for v in left if arrived(v[3], t - margin) and arrived(v[4], t - margin)]
            if pick:
                task = pick[0]
                left.remove(task)
                settle(task[3])
                settle(task[4])
                prog.append(("load", len(tasks)))
                ready_at[len(tasks)] = t + 1.7 if task[0] < chunks - 1 else t
                tasks.append(task[:3])
                continue
        if computed < len(tasks) and ready_at[computed] <= t:
            prog.append(("compute", computed))
            j = tasks[computed][0]
            t += block_us
            computed += 1
            parts[j] = parts.get(j, 0) + 1
            if parts[j] == 4:
                done.add(("C", j))
            continue
        later = [v for n, v in at.items() if n in eager and n not in done]
        later += [e for link in RATE for e in out[link] if e > t]
        later += [v for k, v in ready_at.items() if k >= computed]
        later += [v + margin for n, v in at.items() if n not in done and v + margin > t]
        later = [v for v in later if v > t]
        if not later:
            break
        t = min(later)
    if waiting or left or computed < len(tasks):
        raise ValueError("plan stuck")
    return prog, tasks, list(sends), t


def body(prog, tasks, names, modes, dims, a_ref, x_ref, y_ref, xg, av, xv, xt, xs, yv, acc, ssem, rsem, lsem, vsem):
    layout, s, kb, half, kk = dims
    chunks = len(layout)
    z, y, i = lax.axis_index("depth"), lax.axis_index("col"), lax.axis_index("row")
    x, c = i // 2, i % 2
    zh, pi = z // 2, z % 2
    nu = (zh + pi) % 2
    zl_peer = 2 * zh + 1 - pi
    zh_peer = 3 - z

    def xat(d):
        return (x + d + 4) % 4

    def yat(d):
        return (y + d + 4) % 4

    dev = {
        "xp": (z, y, 2 * xat(1) + c),
        "xm": (z, y, 2 * xat(-1) + c),
        "yp": (z, yat(1), i),
        "ym": (z, yat(-1), i),
        "zl": (zl_peer, y, i),
        "zh": (zh_peer, y, i),
        "dd": (z, y, 2 * x + 1 - c),
    }

    def cols(j, part):
        return pl.ds(pl.multiple_of(part * half + layout[j][1], 128), layout[j][2])

    def lane(j):
        return pl.ds(0, layout[j][2])

    def xin(j, part):
        return x_ref.at[layout[j][0], :, cols(j, part)]

    def xgat(j, block, rows):
        if j == chunks - 1:
            return xt.at[block, rows]
        return xg.at[j, block, rows, lane(j)]

    rows_a = s // A_PIECES

    def arow(which, q):
        return pl.ds(pl.multiple_of(which * s + q * rows_a, 16), rows_a)

    def krow(core, first, count):
        return pl.ds(pl.multiple_of((4 * core + first) * s, 16), count * s)

    def yrow(which):
        return pl.ds(pl.multiple_of(which * s, 16), s)

    def ends(name, recv):
        kind = name[0]
        if kind in ("AL", "AR1", "AL1", "AR2", "AL2"):
            q = name[-1]
            if kind == "AL":
                who = 1 - pi if recv else pi
                ref = av.at[y, arow(who, q)]
                return ref, ref, "zl"
            right = kind in ("AR1", "AR2")
            step = (-1 if right else 1) if recv else 0
            if kind in ("AR1", "AL1"):
                who = pi if name[1] == 0 else 1 - pi
                ref = av.at[yat(step), arow(who, q)]
            else:
                who = pi if right else 1 - pi
                ref = av.at[yat(step + (-1 if right else 1)), arow(who, q)]
            return ref, ref, "yp" if right else "ym"
        j = name[1]
        if kind == "L":
            ref = xgat(j, x, krow(c, zl_peer if recv else z, 1))
            return (ref if recv else xin(j, 1 - nu)), ref, "zl"
        if kind == "Y":
            part = 1 - nu if recv else nu
            ref = y_ref.at[layout[j][0], :, cols(j, part)]
            return yv.at[j, :, lane(j)], ref, "zl"
        if kind == "D":
            ref = xgat(j, xat(name[2]), krow(1 - c if recv else c, 0, 4))
            return ref, ref, "dd"
        own, pair, other = krow(c, z, 1), krow(c, 2 * zh, 2), krow(c, 2 * (1 - zh), 2)
        if kind == "H":
            if modes[j] == "b":
                at = z if name[2] == 0 else zl_peer
                ref = xgat(j, x, krow(c, 3 - at if recv else at, 1))
                return (xin(j, nu) if name[2] == 0 and not recv else ref), ref, "zh"
            ref = xgat(j, xat(name[2]), other if recv else pair)
            return ref, ref, "zh"
        right = kind[0] == "R"
        link = "xp" if right else "xm"
        step = (-1 if right else 1) if recv else 0
        if modes[j] == "b":
            parts = (pair, other)
        else:
            parts = (own, krow(c, zl_peer, 1))
        if kind[1] == "1":
            ref = xgat(j, xat(step), parts[name[2]])
            direct = modes[j] == "a" and name[2] == 0 and not recv
            return (xin(j, nu) if direct else ref), ref, link
        ref = xgat(j, xat(step + (-1 if right else 1)), parts[0 if right else 1])
        return ref, ref, link

    index = {n: k for k, n in enumerate(names)}

    def remote(name, recv=False):
        src, dst, link = ends(name, recv)
        return pltpu.make_async_remote_copy(
            src_ref=src, dst_ref=dst, send_sem=ssem.at[index[name]], recv_sem=rsem.at[index[name]],
            device_id=dev[link], device_id_type=MESH)

    def stage_in(j):
        dst = xgat(j, x, krow(c, z, 1)) if j == chunks - 1 else xs.at[j, :, lane(j)]
        return pltpu.make_async_copy(xin(j, nu), dst, lsem.at[j])

    def stage_out(j):
        return pltpu.make_async_copy(xs.at[j, :, lane(j)], xgat(j, x, krow(c, z, 1)), lsem.at[chunks + j])

    def a_in():
        return pltpu.make_async_copy(a_ref, av.at[y, yrow(pi)], lsem.at[2 * chunks])

    def load(task):
        j, axis, e = tasks[task]
        slot = task % SLOTS
        block = yat(e) if axis == "y" else xat(e)
        return pltpu.make_async_copy(xgat(j, block, pl.ds(0, kb)), xv.at[slot, :, lane(j)], vsem.at[slot])

    barrier = pltpu.get_barrier_semaphore()
    for peer in dev.values():
        pl.semaphore_signal(barrier, inc=1, device_id=peer, device_id_type=MESH)
    for j in range(chunks):
        stage_in(j).start()
    a_in().start()
    pl.semaphore_wait(barrier, len(dev))

    staged = [False]

    def finish_stage():
        for j in range(chunks - 1):
            stage_in(j).wait()
            stage_out(j).start()
        staged[0] = True

    received = set()
    parts = [0] * chunks
    for op, what in prog:
        if op == "start":
            remote(what).start()
        elif op == "load":
            if tasks[what][0] < chunks - 1:
                load(what).start()
        elif op == "wait":
            if not staged[0]:
                finish_stage()
            if what[0] == "S":
                (stage_in if what[1] == chunks - 1 else stage_out)(what[1]).wait()
            elif what[0] == "AS":
                a_in().wait()
            else:
                remote(what, True).wait_recv()
                received.add(what)
        else:
            j, axis, e = tasks[what]
            slot = what % SLOTS
            wide = lane(j)
            if j < chunks - 1:
                load(what).wait()
            if parts[j] == 0:
                acc[j, :, wide] = jnp.zeros((2 * s, layout[j][2]), jnp.float32)
            block = yat(e) if axis == "y" else xat(e)

            def rhs(lanes, slot=slot, block=block, j=j, wide=wide):
                return xt[block, lanes, :] if j == chunks - 1 else xv[slot, lanes, wide]

            def step(k, carry, rhs=rhs, block=block, j=j, wide=wide):
                lanes = pl.ds(pl.multiple_of(k * kk, 128), kk)
                acc[j, :, wide] += jnp.dot(av[block, :, lanes], rhs(lanes), preferred_element_type=jnp.float32)
                return carry

            lax.fori_loop(0, kb // kk, step, 0)
            parts[j] += 1
            if parts[j] == 4:
                yv[j, :, wide] = acc[j, yrow(1 - pi), wide].astype(yv.dtype)
                y_ref[layout[j][0], :, cols(j, nu)] = acc[j, yrow(pi), wide].astype(y_ref.dtype)

    for name in names:
        if name not in received:
            remote(name, True).wait_recv()
    for name in names:
        remote(name).wait_send()


def solution(mesh):
    def local(a, x):
        rhs, s, xc = x.shape
        kb = a.shape[1]
        half = xc // 2
        width = 256 if half % 256 == 0 else 128
        layout = [(r, at, width) for r in range(rhs) for at in range(0, half, width)]
        if width == 256:
            r, at, _ = layout.pop()
            layout += [(r, at, 128), (r, at + 128, 128)]
        chunks = len(layout)
        modes = (MODES * chunks)[:chunks]
        kk = 1024 if kb % 1024 == 0 else 256
        units = [2 * s * w for _, _, w in layout]
        prog, tasks, names, _ = make_plan(units, modes, 2 * s * kb // A_PIECES, BLOCK_US)
        dims = (layout, s, kb, half, kk)
        any_spec = pl.BlockSpec(memory_space=pl.ANY)
        y, _ = pl.pallas_call(
            functools.partial(body, prog, tasks, names, modes, dims),
            out_shape=(pltpu.VMEM(x.shape, x.dtype), jax.ShapeDtypeStruct((chunks, 4, kb, width), x.dtype)),
            in_specs=[any_spec, any_spec],
            out_specs=(pl.BlockSpec(memory_space=pltpu.VMEM), any_spec),
            scratch_shapes=[
                pltpu.VMEM((4, 2 * s, kb), a.dtype),
                pltpu.VMEM((SLOTS, kb, width), x.dtype),
                pltpu.VMEM((4, kb, layout[-1][2]), x.dtype),
                pltpu.VMEM((chunks, s, width), x.dtype),
                pltpu.VMEM((chunks, s, width), x.dtype),
                pltpu.VMEM((chunks, 2 * s, width), jnp.float32),
                pltpu.SemaphoreType.DMA((len(names),)),
                pltpu.SemaphoreType.DMA((len(names),)),
                pltpu.SemaphoreType.DMA((2 * chunks + 1,)),
                pltpu.SemaphoreType.DMA((SLOTS,)),
            ],
            compiler_params=pltpu.CompilerParams(collective_id=0, has_side_effects=True, vmem_limit_bytes=54 * 1024 * 1024),
        )(a, x)
        return y

    spec_a = P(("row", "depth"), "col")
    spec_x = P(None, ("row", "depth"), "col")
    return jax.shard_map(local, mesh=mesh, in_specs=(spec_a, spec_x), out_specs=spec_x, check_vma=False)
```

```python
import functools

import jax
import jax.numpy as jnp
from jax import lax
from jax.experimental import pallas as pl
from jax.experimental.pallas import tpu as pltpu
from jax.sharding import PartitionSpec as P

MESH = pl.DeviceIdType.MESH
MODES = "babbabaababbb"
A_PIECES = 4
SLOTS = 5
DEPTH_Q = 3
TAIL_CHUNKS = 4
MARGIN = 2.0
PLAN_LAT = 4.5
BLOCK_US = 1.6
RATE = {"xp": 46.0e3, "xm": 46.0e3, "yp": 46.0e3, "ym": 46.0e3, "zl": 46.0e3, "zh": 46.0e3, "dd": 300.0e3}
LAT = {"dd": 2.5}


def make_plan(units, modes, a_unit, block_us):
    sends = {}
    chunks = len(units)

    def add(name, link, size, deps, key):
        sends[name] = (link, size, frozenset(deps), key)

    need = {}
    for j in range(chunks):
        S, L, unit = ("S", j), ("L", j), units[j]
        add(L, "zl", unit, [], j - 1)
        if modes[j] == "b":
            add(("H", j, 0), "zh", unit, [], j - 1.5)
            add(("H", j, 1), "zh", unit, [L], j - 1.5)
            h = [("H", j, 0), ("H", j, 1)]
            for way, link in (("R", "xp"), ("L", "xm")):
                add((way + "1", j, 0), link, 2 * unit, [S, L], (j, 1))
                add((way + "1", j, 1), link, 2 * unit, h, (j, 1))
            add(("R2", j), "xp", 2 * unit, [("R1", j, 0)], (j, 0))
            add(("L2", j), "xm", 2 * unit, [("L1", j, 1)], (j, 0))
            got = {0: [S, L] + h, -1: [("R1", j, 0), ("R1", j, 1)], 1: [("L1", j, 0), ("L1", j, 1)], 2: [("R2", j), ("L2", j)]}
        else:
            for way, link in (("R", "xp"), ("L", "xm")):
                add((way + "1", j, 0), link, unit, [], (j, 1))
                add((way + "1", j, 1), link, unit, [L], (j, 1))
            add(("R2", j), "xp", unit, [("R1", j, 0)], (j, 0))
            add(("L2", j), "xm", unit, [("L1", j, 1)], (j, 0))
            pre = {0: [S, L], -1: [("R1", j, 0), ("R1", j, 1)], 1: [("L1", j, 0), ("L1", j, 1)], 2: [("R2", j), ("L2", j)]}
            got = {}
            for d in (0, -1, 1, 2):
                add(("H", j, d), "zh", 2 * unit, pre[d], j)
                got[d] = pre[d] + [("H", j, d)]
        for d in (0, -1, 1, 2):
            add(("D", j, d), "dd", 4 * unit, got[d], j)
            need[j, d] = got[d] + [("D", j, d)]
        add(("Y", j), "zl", unit, [("C", j)], j)
    a_need = {0: [("AS",)], 1: [], -1: [], 2: []}
    for q in range(A_PIECES):
        add(("AL", q), "zl", a_unit, [("AS",)], 0.75 * q)
        for t in (0, 1):
            dep = [("AS",)] if t == 0 else [("AL", q)]
            add(("AR1", t, q), "yp", a_unit, dep, 4 * t + q)
            add(("AL1", t, q), "ym", a_unit, dep, 4 * t + q)
            a_need[-1].append(("AR1", t, q))
            a_need[1].append(("AL1", t, q))
        add(("AR2", q), "yp", a_unit, [("AR1", 0, q)], 8 + q)
        add(("AL2", q), "ym", a_unit, [("AL1", 1, q)], 8 + q)
        a_need[0].append(("AL", q))
        a_need[2] += [("AR2", q), ("AL2", q)]
    a_all = sum(a_need.values(), [])

    tasks = []
    left = []
    for j in range(chunks):
        for e in (0, -1, 1, 2):
            if j < chunks - TAIL_CHUNKS:
                left.append((j, "y", e, sum((need[j, d] for d in (0, -1, 1, 2)), []), a_need[e]))
            else:
                left.append((j, "x", e, need[j, e], a_all))

    prog = []
    t = 0.0
    at = {("AS",): 3.0}
    for j in range(chunks):
        at[("S", j)] = 2.5 + 0.3 * j
    eager = set().union(*(v[2] for v in sends.values()))
    done = set()
    waiting = dict(sends)
    busy = {k: 0.0 for k in RATE}
    out = {k: [] for k in RATE}
    ready_at = {}
    computed = 0
    parts = {}

    def arrived(events, when):
        return all(n in done or at.get(n, 1e9) <= when for n in events)

    def settle(events):
        for n in events:
            if n not in done:
                done.add(n)
                prog.append(("wait", n))

    while True:
        for link in RATE:
            out[link] = [e for e in out[link] if e > t]
            while len(out[link]) < DEPTH_Q:
                ready = [n for n, v in waiting.items() if v[0] == link and v[2] <= done]
                if not ready:
                    break
                name = min(ready, key=lambda n: (waiting[n][3], str(n)))
                size = waiting.pop(name)[1]
                busy[link] = max(busy[link], t + 0.2) + size / RATE[link]
                out[link].append(busy[link])
                at[name] = busy[link] + LAT.get(link, PLAN_LAT)
                prog.append(("start", name))
        now = sorted((v, str(n), n) for n, v in at.items() if n in eager and n not in done and v <= t)
        if now:
            settle([now[0][2]])
            continue
        margin = MARGIN if len(left) > 4 * TAIL_CHUNKS else 0.0
        if len(tasks) - computed < SLOTS:
            pick = [v for v in left if arrived(v[3], t - margin) and arrived(v[4], t - margin)]
            if pick:
                task = pick[0]
                left.remove(task)
                settle(task[3])
                settle(task[4])
                prog.append(("load", len(tasks)))
                ready_at[len(tasks)] = t + 1.7 if task[0] < chunks - 1 else t
                tasks.append(task[:3])
                continue
        if computed < len(tasks) and ready_at[computed] <= t:
            prog.append(("compute", computed))
            j = tasks[computed][0]
            t += block_us
            computed += 1
            parts[j] = parts.get(j, 0) + 1
            if parts[j] == 4:
                done.add(("C", j))
            continue
        later = [v for n, v in at.items() if n in eager and n not in done]
        later += [e for link in RATE for e in out[link] if e > t]
        later += [v for k, v in ready_at.items() if k >= computed]
        later += [v + margin for n, v in at.items() if n not in done and v + margin > t]
        later = [v for v in later if v > t]
        if not later:
            break
        t = min(later)
    if waiting or left or computed < len(tasks):
        raise ValueError("plan stuck")
    return prog, tasks, list(sends), t


def body(prog, tasks, names, modes, dims, a_ref, x_ref, y_ref, xg, av, xv, xt, xs, yv, acc, ssem, rsem, lsem, vsem):
    layout, s, kb, half, kk = dims
    chunks = len(layout)
    z, y, i = lax.axis_index("depth"), lax.axis_index("col"), lax.axis_index("row")
    x, c = i // 2, i % 2
    zh, pi = z // 2, z % 2
    nu = (zh + pi) % 2
    zl_peer = 2 * zh + 1 - pi
    zh_peer = 3 - z

    def xat(d):
        return (x + d + 4) % 4

    def yat(d):
        return (y + d + 4) % 4

    dev = {
        "xp": (z, y, 2 * xat(1) + c),
        "xm": (z, y, 2 * xat(-1) + c),
        "yp": (z, yat(1), i),
        "ym": (z, yat(-1), i),
        "zl": (zl_peer, y, i),
        "zh": (zh_peer, y, i),
        "dd": (z, y, 2 * x + 1 - c),
    }

    def cols(j, part):
        return pl.ds(pl.multiple_of(part * half + layout[j][1], 128), layout[j][2])

    def lane(j):
        return pl.ds(0, layout[j][2])

    def xin(j, part):
        return x_ref.at[layout[j][0], :, cols(j, part)]

    def xgat(j, block, rows):
        if j == chunks - 1:
            return xt.at[block, rows]
        return xg.at[j, block, rows, lane(j)]

    rows_a = s // A_PIECES

    def arow(which, q):
        return pl.ds(pl.multiple_of(which * s + q * rows_a, 16), rows_a)

    def krow(core, first, count):
        return pl.ds(pl.multiple_of((4 * core + first) * s, 16), count * s)

    def yrow(which):
        return pl.ds(pl.multiple_of(which * s, 16), s)

    def ends(name, recv):
        kind = name[0]
        if kind in ("AL", "AR1", "AL1", "AR2", "AL2"):
            q = name[-1]
            if kind == "AL":
                who = 1 - pi if recv else pi
                ref = av.at[y, arow(who, q)]
                return ref, ref, "zl"
            right = kind in ("AR1", "AR2")
            step = (-1 if right else 1) if recv else 0
            if kind in ("AR1", "AL1"):
                who = pi if name[1] == 0 else 1 - pi
                ref = av.at[yat(step), arow(who, q)]
            else:
                who = pi if right else 1 - pi
                ref = av.at[yat(step + (-1 if right else 1)), arow(who, q)]
            return ref, ref, "yp" if right else "ym"
        j = name[1]
        if kind == "L":
            ref = xgat(j, x, krow(c, zl_peer if recv else z, 1))
            return (ref if recv else xin(j, 1 - nu)), ref, "zl"
        if kind == "Y":
            part = 1 - nu if recv else nu
            ref = y_ref.at[layout[j][0], :, cols(j, part)]
            return yv.at[j, :, lane(j)], ref, "zl"
        if kind == "D":
            ref = xgat(j, xat(name[2]), krow(1 - c if recv else c, 0, 4))
            return ref, ref, "dd"
        own, pair, other = krow(c, z, 1), krow(c, 2 * zh, 2), krow(c, 2 * (1 - zh), 2)
        if kind == "H":
            if modes[j] == "b":
                at = z if name[2] == 0 else zl_peer
                ref = xgat(j, x, krow(c, 3 - at if recv else at, 1))
                return (xin(j, nu) if name[2] == 0 and not recv else ref), ref, "zh"
            ref = xgat(j, xat(name[2]), other if recv else pair)
            return ref, ref, "zh"
        right = kind[0] == "R"
        link = "xp" if right else "xm"
        step = (-1 if right else 1) if recv else 0
        if modes[j] == "b":
            parts = (pair, other)
        else:
            parts = (own, krow(c, zl_peer, 1))
        if kind[1] == "1":
            ref = xgat(j, xat(step), parts[name[2]])
            direct = modes[j] == "a" and name[2] == 0 and not recv
            return (xin(j, nu) if direct else ref), ref, link
        ref = xgat(j, xat(step + (-1 if right else 1)), parts[0 if right else 1])
        return ref, ref, link

    index = {n: k for k, n in enumerate(names)}

    def remote(name, recv=False):
        src, dst, link = ends(name, recv)
        return pltpu.make_async_remote_copy(
            src_ref=src, dst_ref=dst, send_sem=ssem.at[index[name]], recv_sem=rsem.at[index[name]],
            device_id=dev[link], device_id_type=MESH)

    def stage_in(j):
        dst = xgat(j, x, krow(c, z, 1)) if j == chunks - 1 else xs.at[j, :, lane(j)]
        return pltpu.make_async_copy(xin(j, nu), dst, lsem.at[j])

    def stage_out(j):
        return pltpu.make_async_copy(xs.at[j, :, lane(j)], xgat(j, x, krow(c, z, 1)), lsem.at[chunks + j])

    def a_in():
        return pltpu.make_async_copy(a_ref, av.at[y, yrow(pi)], lsem.at[2 * chunks])

    def load(task):
        j, axis, e = tasks[task]
        slot = task % SLOTS
        block = yat(e) if axis == "y" else xat(e)
        return pltpu.make_async_copy(xgat(j, block, pl.ds(0, kb)), xv.at[slot, :, lane(j)], vsem.at[slot])

    barrier = pltpu.get_barrier_semaphore()
    for peer in dev.values():
        pl.semaphore_signal(barrier, inc=1, device_id=peer, device_id_type=MESH)
    for j in range(chunks):
        stage_in(j).start()
    a_in().start()
    pl.semaphore_wait(barrier, len(dev))

    staged = [False]

    def finish_stage():
        for j in range(chunks - 1):
            stage_in(j).wait()
            stage_out(j).start()
        staged[0] = True

    received = set()
    parts = [0] * chunks
    for op, what in prog:
        if op == "start":
            remote(what).start()
        elif op == "load":
            if tasks[what][0] < chunks - 1:
                load(what).start()
        elif op == "wait":
            if not staged[0]:
                finish_stage()
            if what[0] == "S":
                (stage_in if what[1] == chunks - 1 else stage_out)(what[1]).wait()
            elif what[0] == "AS":
                a_in().wait()
            else:
                remote(what, True).wait_recv()
                received.add(what)
        else:
            j, axis, e = tasks[what]
            slot = what % SLOTS
            wide = lane(j)
            if j < chunks - 1:
                load(what).wait()
            if parts[j] == 0:
                acc[j, :, wide] = jnp.zeros((2 * s, layout[j][2]), jnp.float32)
            block = yat(e) if axis == "y" else xat(e)

            def rhs(lanes, slot=slot, block=block, j=j, wide=wide):
                return xt[block, lanes, :] if j == chunks - 1 else xv[slot, lanes, wide]

            def step(k, carry, rhs=rhs, block=block, j=j, wide=wide):
                lanes = pl.ds(pl.multiple_of(k * kk, 128), kk)
                acc[j, :, wide] += jnp.dot(av[block, :, lanes], rhs(lanes), preferred_element_type=jnp.float32)
                return carry

            lax.fori_loop(0, kb // kk, step, 0)
            parts[j] += 1
            if parts[j] == 4:
                yv[j, :, wide] = acc[j, yrow(1 - pi), wide].astype(yv.dtype)
                y_ref[layout[j][0], :, cols(j, nu)] = acc[j, yrow(pi), wide].astype(y_ref.dtype)

    for name in names:
        if name not in received:
            remote(name, True).wait_recv()
    for name in names:
        remote(name).wait_send()


def solution(mesh):
    def local(a, x):
        rhs, s, xc = x.shape
        kb = a.shape[1]
        half = xc // 2
        width = 256 if half % 256 == 0 else 128
        layout = [(r, at, width) for r in range(rhs) for at in range(0, half, width)]
        if width == 256:
            r, at, _ = layout.pop()
            layout += [(r, at, 128), (r, at + 128, 128)]
        chunks = len(layout)
        modes = (MODES * chunks)[:chunks]
        kk = 1024 if kb % 1024 == 0 else 256
        units = [2 * s * w for _, _, w in layout]
        prog, tasks, names, _ = make_plan(units, modes, 2 * s * kb // A_PIECES, BLOCK_US)
        dims = (layout, s, kb, half, kk)
        any_spec = pl.BlockSpec(memory_space=pl.ANY)
        y, _ = pl.pallas_call(
            functools.partial(body, prog, tasks, names, modes, dims),
            out_shape=(pltpu.VMEM(x.shape, x.dtype), jax.ShapeDtypeStruct((chunks, 4, kb, width), x.dtype)),
            in_specs=[any_spec, any_spec],
            out_specs=(pl.BlockSpec(memory_space=pltpu.VMEM), any_spec),
            scratch_shapes=[
                pltpu.VMEM((4, 2 * s, kb), a.dtype),
                pltpu.VMEM((SLOTS, kb, width), x.dtype),
                pltpu.VMEM((4, kb, layout[-1][2]), x.dtype),
                pltpu.VMEM((chunks, s, width), x.dtype),
                pltpu.VMEM((chunks, s, width), x.dtype),
                pltpu.VMEM((chunks, 2 * s, width), jnp.float32),
                pltpu.SemaphoreType.DMA((len(names),)),
                pltpu.SemaphoreType.DMA((len(names),)),
                pltpu.SemaphoreType.DMA((2 * chunks + 1,)),
                pltpu.SemaphoreType.DMA((SLOTS,)),
            ],
            compiler_params=pltpu.CompilerParams(collective_id=0, has_side_effects=True, vmem_limit_bytes=54 * 1024 * 1024),
        )(a, x)
        return y

    spec_a = P(("row", "depth"), "col")
    spec_x = P(None, ("row", "depth"), "col")
    return jax.shard_map(local, mesh=mesh, in_specs=(spec_a, spec_x), out_specs=spec_x, check_vma=False)
```

```python
import functools

import jax
import jax.numpy as jnp
from jax import lax
from jax.experimental import pallas as pl
from jax.experimental.pallas import tpu as pltpu
from jax.sharding import PartitionSpec as P

MESH = pl.DeviceIdType.MESH
MODES = "babbabaababbb"
A_PIECES = 4
SLOTS = 5
DEPTH_Q = 3
TAIL_CHUNKS = 4
MARGIN = 2.0
PLAN_LAT = 3.5
BLOCK_US = 1.6
RATE = {"xp": 46.0e3, "xm": 46.0e3, "yp": 46.0e3, "ym": 46.0e3, "zl": 46.0e3, "zh": 46.0e3, "dd": 300.0e3}
LAT = {"dd": 2.5}
WHOLE_K = 8
KEYS = (-9.0, -1.5, -0.6, 1.2)


def make_plan(units, modes, a_unit, block_us):
    sends = {}
    chunks = len(units)

    def add(name, link, size, deps, key):
        sends[name] = (link, size, frozenset(deps), key)

    need = {}
    for j in range(chunks):
        S, L, unit = ("S", j), ("L", j), units[j]
        add(L, "zl", unit, [], j - 1)
        if modes[j] in "bc":
            add(("H", j, 0), "zh", unit, [], j + KEYS[0])
            add(("H", j, 1), "zh", unit, [L], j + KEYS[0])
            h = [("H", j, 0), ("H", j, 1)]
            for way, link in (("R", "xp"), ("L", "xm")):
                add((way + "1", j, 0), link, 2 * unit, [S, L], (j + KEYS[2], 1))
                add((way + "1", j, 1), link, 2 * unit, h, (j + KEYS[2], 1))
            far = [("R2", j), ("L2", j)]
            if modes[j] == "b":
                add(far[0], "xp", 2 * unit, [("R1", j, 0)], (j + KEYS[3], 0))
                add(far[1], "xm", 2 * unit, [("L1", j, 1)], (j + KEYS[3], 0))
            else:
                add(far[0], "xp", unit, [("R1", j, 0)], (j + KEYS[3], 0))
                add(far[1], "xm", unit, [("L1", j, 0)], (j + KEYS[3], 0))
                add(("H", j, 2), "zh", 2 * unit, far, j + KEYS[1])
                far = far + [("H", j, 2)]
            got = {0: [S, L] + h, -1: [("R1", j, 0), ("R1", j, 1)], 1: [("L1", j, 0), ("L1", j, 1)], 2: far}
        elif modes[j] == "m":
            add(("H", j, 9), "zh", unit, [L], j + KEYS[0])
            for way, link in (("R", "xp"), ("L", "xm")):
                add((way + "1", j, 0), link, unit, [], (j, 1))
                add((way + "1", j, 1), link, unit, [L], (j, 1))
                add((way + "1", j, 2), link, unit, [("H", j, 9)], (j, 1))
                add((way + "3", j), link, unit // 2, [(way + "1", j, 2)], (j, 0))
            add(("R2", j), "xp", unit, [("R1", j, 0)], (j, 0))
            add(("L2", j), "xm", unit, [("L1", j, 1)], (j, 0))
            for d, dep in ((0, S), (-1, ("R1", j, 0)), (1, ("L1", j, 0)), (2, ("R2", j))):
                add(("H", j, d), "zh", unit, [dep], j + KEYS[1])
            got = {0: [S, L, ("H", j, 9)], -1: [("R1", j, k) for k in range(3)], 1: [("L1", j, k) for k in range(3)],
                   2: [("R2", j), ("L2", j), ("R3", j), ("L3", j)]}
            for d in got:
                got[d] = got[d] + [("H", j, d)]
        else:
            for way, link in (("R", "xp"), ("L", "xm")):
                add((way + "1", j, 0), link, unit, [], (j, 1))
                add((way + "1", j, 1), link, unit, [L], (j, 1))
            add(("R2", j), "xp", unit, [("R1", j, 0)], (j, 0))
            add(("L2", j), "xm", unit, [("L1", j, 1)], (j, 0))
            pre = {0: [S, L], -1: [("R1", j, 0), ("R1", j, 1)], 1: [("L1", j, 0), ("L1", j, 1)], 2: [("R2", j), ("L2", j)]}
            got = {}
            for d in (0, -1, 1, 2):
                add(("H", j, d), "zh", 2 * unit, pre[d], j + KEYS[1])
                got[d] = pre[d] + [("H", j, d)]
        for d in (0, -1, 1, 2):
            add(("D", j, d), "dd", 4 * unit, got[d], j)
            need[j, d] = got[d] + [("D", j, d)]
        add(("Y", j), "zl", unit, [("C", j)], j)
    a_need = {0: [("AS",)], 1: [], -1: [], 2: []}
    for q in range(A_PIECES):
        add(("AL", q), "zl", a_unit, [("AS",)], 0.75 * q)
        for t in (0, 1):
            dep = [("AS",)] if t == 0 else [("AL", q)]
            add(("AR1", t, q), "yp", a_unit, dep, 4 * t + q)
            add(("AL1", t, q), "ym", a_unit, dep, 4 * t + q)
            a_need[-1].append(("AR1", t, q))
            a_need[1].append(("AL1", t, q))
        add(("AR2", q), "yp", a_unit, [("AR1", 0, q)], 8 + q)
        add(("AL2", q), "ym", a_unit, [("AL1", 1, q)], 8 + q)
        a_need[0].append(("AL", q))
        a_need[2] += [("AR2", q), ("AL2", q)]
    a_all = sum(a_need.values(), [])

    tasks = []
    left = []
    for j in range(chunks):
        for e in (0, -1, 1, 2):
            if j < chunks - TAIL_CHUNKS:
                left.append((j, "y", e, sum((need[j, d] for d in (0, -1, 1, 2)), []), a_need[e]))
            else:
                left.append((j, "x", e, need[j, e], a_all))

    prog = []
    t = 0.0
    at = {("AS",): 3.0}
    for j in range(chunks):
        at[("S", j)] = 2.5 + 0.3 * j
    eager = set().union(*(v[2] for v in sends.values()))
    done = set()
    waiting = dict(sends)
    busy = {k: 0.0 for k in RATE}
    out = {k: [] for k in RATE}
    ready_at = {}
    computed = 0
    parts = {}

    def arrived(events, when):
        return all(n in done or at.get(n, 1e9) <= when for n in events)

    def settle(events):
        for n in events:
            if n not in done:
                done.add(n)
                prog.append(("wait", n))

    while True:
        for link in RATE:
            out[link] = [e for e in out[link] if e > t]
            while len(out[link]) < DEPTH_Q:
                ready = [n for n, v in waiting.items() if v[0] == link and v[2] <= done]
                if not ready:
                    break
                name = min(ready, key=lambda n: (waiting[n][3], str(n)))
                size = waiting.pop(name)[1]
                busy[link] = max(busy[link], t + 0.2) + size / RATE[link]
                out[link].append(busy[link])
                at[name] = busy[link] + LAT.get(link, PLAN_LAT)
                prog.append(("start", name))
        now = sorted((v, str(n), n) for n, v in at.items() if n in eager and n not in done and v <= t)
        if now:
            settle([now[0][2]])
            continue
        margin = MARGIN if len(left) > 4 * TAIL_CHUNKS else 0.0
        if len(tasks) - computed < SLOTS:
            pick = [v for v in left if arrived(v[3], t - margin) and arrived(v[4], t - margin)]
            if pick:
                task = pick[0]
                left.remove(task)
                settle(task[3])
                settle(task[4])
                prog.append(("load", len(tasks)))
                ready_at[len(tasks)] = t + 1.7 if task[0] < chunks - 1 else t
                tasks.append(task[:3])
                continue
        if computed < len(tasks) and ready_at[computed] <= t:
            prog.append(("compute", computed))
            j = tasks[computed][0]
            t += block_us
            computed += 1
            parts[j] = parts.get(j, 0) + 1
            if parts[j] == 4:
                done.add(("C", j))
            continue
        later = [v for n, v in at.items() if n in eager and n not in done]
        later += [e for link in RATE for e in out[link] if e > t]
        later += [v for k, v in ready_at.items() if k >= computed]
        later += [v + margin for n, v in at.items() if n not in done and v + margin > t]
        later = [v for v in later if v > t]
        if not later:
            break
        t = min(later)
    if waiting or left or computed < len(tasks):
        raise ValueError("plan stuck")
    return prog, tasks, list(sends), t


def body(prog, tasks, names, modes, dims, a_ref, x_ref, y_ref, xg, av, xv, xt, xs, yv, acc, ssem, rsem, lsem, vsem):
    layout, s, kb, half, kk = dims
    chunks = len(layout)
    z, y, i = lax.axis_index("depth"), lax.axis_index("col"), lax.axis_index("row")
    x, c = i // 2, i % 2
    zh, pi = z // 2, z % 2
    nu = (zh + pi) % 2
    zl_peer = 2 * zh + 1 - pi
    zh_peer = 3 - z

    def xat(d):
        return (x + d + 4) % 4

    def yat(d):
        return (y + d + 4) % 4

    dev = {
        "xp": (z, y, 2 * xat(1) + c),
        "xm": (z, y, 2 * xat(-1) + c),
        "yp": (z, yat(1), i),
        "ym": (z, yat(-1), i),
        "zl": (zl_peer, y, i),
        "zh": (zh_peer, y, i),
        "dd": (z, y, 2 * x + 1 - c),
    }

    def cols(j, part):
        return pl.ds(pl.multiple_of(part * half + layout[j][1], 128), layout[j][2])

    def lane(j):
        return pl.ds(0, layout[j][2])

    def xin(j, part):
        return x_ref.at[layout[j][0], :, cols(j, part)]

    def xgat(j, block, rows):
        if j == chunks - 1:
            return xt.at[block, rows]
        return xg.at[j, block, rows, lane(j)]

    rows_a = s // A_PIECES

    def arow(which, q):
        return pl.ds(pl.multiple_of(which * s + q * rows_a, 16), rows_a)

    def krow(core, first, count):
        return pl.ds(pl.multiple_of((4 * core + first) * s, 16), count * s)

    def yrow(which):
        return pl.ds(pl.multiple_of(which * s, 16), s)

    def ends(name, recv):
        kind = name[0]
        if kind in ("AL", "AR1", "AL1", "AR2", "AL2"):
            q = name[-1]
            if kind == "AL":
                who = 1 - pi if recv else pi
                ref = av.at[y, arow(who, q)]
                return ref, ref, "zl"
            right = kind in ("AR1", "AR2")
            step = (-1 if right else 1) if recv else 0
            if kind in ("AR1", "AL1"):
                who = pi if name[1] == 0 else 1 - pi
                ref = av.at[yat(step), arow(who, q)]
            else:
                who = pi if right else 1 - pi
                ref = av.at[yat(step + (-1 if right else 1)), arow(who, q)]
            return ref, ref, "yp" if right else "ym"
        j = name[1]
        if kind == "L":
            ref = xgat(j, x, krow(c, zl_peer if recv else z, 1))
            return (ref if recv else xin(j, 1 - nu)), ref, "zl"
        if kind == "Y":
            part = 1 - nu if recv else nu
            ref = y_ref.at[layout[j][0], :, cols(j, part)]
            return yv.at[j, :, lane(j)], ref, "zl"
        if kind == "D":
            ref = xgat(j, xat(name[2]), krow(1 - c if recv else c, 0, 4))
            return ref, ref, "dd"
        own, pair, other = krow(c, z, 1), krow(c, 2 * zh, 2), krow(c, 2 * (1 - zh), 2)
        if kind == "H":
            if modes[j] in "bc" and name[2] != 2:
                at = z if name[2] == 0 else zl_peer
                ref = xgat(j, x, krow(c, 3 - at if recv else at, 1))
                return (xin(j, nu) if name[2] == 0 and not recv else ref), ref, "zh"
            if modes[j] == "m":
                at, block = (zl_peer, x) if name[2] == 9 else (z, xat(name[2]))
                ref = xgat(j, block, krow(c, 3 - at if recv else at, 1))
                return ref, ref, "zh"
            ref = xgat(j, xat(name[2]), other if recv else pair)
            return ref, ref, "zh"
        right = kind[0] == "R"
        link = "xp" if right else "xm"
        step = (-1 if right else 1) if recv else 0
        if modes[j] == "b" or (modes[j] == "c" and kind[1] == "1"):
            parts = (pair, other)
        else:
            parts = (own, krow(c, zl_peer, 1), krow(c, 3 - zl_peer, 1))
        if kind[1] == "3":
            at = (4 * c + 3 - zl_peer) * s + (0 if right else s // 2)
            ref = xgat(j, xat(step + (-1 if right else 1)), pl.ds(pl.multiple_of(at, 16), s // 2))
            return ref, ref, link
        if kind[1] == "1":
            ref = xgat(j, xat(step), parts[name[2]])
            direct = modes[j] in "am" and name[2] == 0 and not recv
            return (xin(j, nu) if direct else ref), ref, link
        ref = xgat(j, xat(step + (-1 if right else 1)), parts[0 if right else 1])
        return ref, ref, link

    index = {n: k for k, n in enumerate(names)}

    def remote(name, recv=False):
        src, dst, link = ends(name, recv)
        return pltpu.make_async_remote_copy(
            src_ref=src, dst_ref=dst, send_sem=ssem.at[index[name]], recv_sem=rsem.at[index[name]],
            device_id=dev[link], device_id_type=MESH)

    def stage_in(j):
        dst = xgat(j, x, krow(c, z, 1)) if j == chunks - 1 else xs.at[j, :, lane(j)]
        return pltpu.make_async_copy(xin(j, nu), dst, lsem.at[j])

    def stage_out(j):
        return pltpu.make_async_copy(xs.at[j, :, lane(j)], xgat(j, x, krow(c, z, 1)), lsem.at[chunks + j])

    def a_in():
        return pltpu.make_async_copy(a_ref, av.at[y, yrow(pi)], lsem.at[2 * chunks])

    def load(task):
        j, axis, e = tasks[task]
        slot = task % SLOTS
        block = yat(e) if axis == "y" else xat(e)
        return pltpu.make_async_copy(xgat(j, block, pl.ds(0, kb)), xv.at[slot, :, lane(j)], vsem.at[slot])

    barrier = pltpu.get_barrier_semaphore()
    for peer in dev.values():
        pl.semaphore_signal(barrier, inc=1, device_id=peer, device_id_type=MESH)
    for j in range(chunks):
        stage_in(j).start()
    a_in().start()
    pl.semaphore_wait(barrier, len(dev))

    staged = [False]

    def finish_stage():
        for j in range(chunks - 1):
            stage_in(j).wait()
            stage_out(j).start()
        staged[0] = True

    received = set()
    parts = [0] * chunks
    for op, what in prog:
        if op == "start":
            if what != ("Y", tasks[-1][0]):
                remote(what).start()
        elif op == "load":
            if tasks[what][0] < chunks - 1:
                load(what).start()
        elif op == "wait":
            if not staged[0]:
                finish_stage()
            if what[0] == "S":
                (stage_in if what[1] == chunks - 1 else stage_out)(what[1]).wait()
            elif what[0] == "AS":
                a_in().wait()
            else:
                remote(what, True).wait_recv()
                received.add(what)
        else:
            j, axis, e = tasks[what]
            slot = what % SLOTS
            wide = lane(j)
            if j < chunks - 1:
                load(what).wait()
            if parts[j] == 0:
                acc[j, :, wide] = jnp.zeros((2 * s, layout[j][2]), jnp.float32)
            block = yat(e) if axis == "y" else xat(e)

            def rhs(lanes, slot=slot, block=block, j=j, wide=wide):
                return xt[block, lanes, :] if j == chunks - 1 else xv[slot, lanes, wide]

            whole = what == len(tasks) - 1 or (what >= len(tasks) - WHOLE_K and layout[j][2] == 256)
            deep = kb if whole else kk

            def step(k, rows, rhs=rhs, block=block, j=j, wide=wide, deep=deep):
                lanes = slice(None) if deep == kb else pl.ds(pl.multiple_of(k * deep, 128), deep)
                acc[j, rows, wide] += jnp.dot(av[block, rows, lanes], rhs(lanes), preferred_element_type=jnp.float32)

            def loop(rows, step=step, deep=deep):
                if deep == kb:
                    step(0, rows)
                else:
                    lax.fori_loop(0, kb // deep, lambda k, carry: (step(k, rows), carry)[1], 0)

            parts[j] += 1
            if what == len(tasks) - 1:
                loop(yrow(1 - pi))
                yv[j, :, wide] = acc[j, yrow(1 - pi), wide].astype(yv.dtype)
                remote(("Y", j)).start()
                loop(yrow(pi))
                y_ref[layout[j][0], :, cols(j, nu)] = acc[j, yrow(pi), wide].astype(y_ref.dtype)
                continue
            loop(slice(None))
            if parts[j] == 4:
                yv[j, :, wide] = acc[j, yrow(1 - pi), wide].astype(yv.dtype)
                y_ref[layout[j][0], :, cols(j, nu)] = acc[j, yrow(pi), wide].astype(y_ref.dtype)

    for name in names:
        if name not in received:
            remote(name, True).wait_recv()
    for name in names:
        remote(name).wait_send()


def solution(mesh):
    def local(a, x):
        rhs, s, xc = x.shape
        kb = a.shape[1]
        half = xc // 2
        width = 256 if half % 256 == 0 else 128
        layout = [(r, at, width) for r in range(rhs) for at in range(0, half, width)]
        if width == 256:
            r, at, _ = layout.pop()
            layout += [(r, at, 128), (r, at + 128, 128)]
        chunks = len(layout)
        modes = (MODES * chunks)[:chunks]
        kk = 1024 if kb % 1024 == 0 else 256
        units = [2 * s * w for _, _, w in layout]
        prog, tasks, names, _ = make_plan(units, modes, 2 * s * kb // A_PIECES, BLOCK_US)
        dims = (layout, s, kb, half, kk)
        any_spec = pl.BlockSpec(memory_space=pl.ANY)
        y, _ = pl.pallas_call(
            functools.partial(body, prog, tasks, names, modes, dims),
            out_shape=(pltpu.VMEM(x.shape, x.dtype), jax.ShapeDtypeStruct((chunks, 4, kb, width), x.dtype)),
            in_specs=[any_spec, any_spec],
            out_specs=(pl.BlockSpec(memory_space=pltpu.VMEM), any_spec),
            scratch_shapes=[
                pltpu.VMEM((4, 2 * s, kb), a.dtype),
                pltpu.VMEM((SLOTS, kb, width), x.dtype),
                pltpu.VMEM((4, kb, layout[-1][2]), x.dtype),
                pltpu.VMEM((chunks, s, width), x.dtype),
                pltpu.VMEM((chunks, s, width), x.dtype),
                pltpu.VMEM((chunks, 2 * s, width), jnp.float32),
                pltpu.SemaphoreType.DMA((len(names),)),
                pltpu.SemaphoreType.DMA((len(names),)),
                pltpu.SemaphoreType.DMA((2 * chunks + 1,)),
                pltpu.SemaphoreType.DMA((SLOTS,)),
            ],
            compiler_params=pltpu.CompilerParams(collective_id=0, has_side_effects=True, vmem_limit_bytes=54 * 1024 * 1024),
        )(a, x)
        return y

    spec_a = P(("row", "depth"), "col")
    spec_x = P(None, ("row", "depth"), "col")
    return jax.shard_map(local, mesh=mesh, in_specs=(spec_a, spec_x), out_specs=spec_x, check_vma=False)
```

```python
import functools

import jax
import jax.numpy as jnp
from jax import lax
from jax.experimental import pallas as pl
from jax.experimental.pallas import tpu as pltpu
from jax.sharding import PartitionSpec as P

MESH = pl.DeviceIdType.MESH
MODES = "babbabaababbb"
A_PIECES = 4
SLOTS = 5
DEPTH_Q = 3
TAIL_CHUNKS = 4
MARGIN = 2.0
PLAN_LAT = 4.5
BLOCK_US = 1.6
RATE = {"xp": 46.0e3, "xm": 46.0e3, "yp": 46.0e3, "ym": 46.0e3, "zl": 46.0e3, "zh": 46.0e3, "dd": 300.0e3}
LAT = {"dd": 2.5}
WHOLE_K = 8
KEYS = (-1.5, 0.0, 0.0, 0.0)


def make_plan(units, modes, a_unit, block_us):
    sends = {}
    chunks = len(units)

    def add(name, link, size, deps, key):
        sends[name] = (link, size, frozenset(deps), key)

    need = {}
    for j in range(chunks):
        S, L, unit = ("S", j), ("L", j), units[j]
        add(L, "zl", unit, [], j - 1)
        if modes[j] in "bc":
            add(("H", j, 0), "zh", unit, [], j + KEYS[0])
            add(("H", j, 1), "zh", unit, [L], j + KEYS[0])
            h = [("H", j, 0), ("H", j, 1)]
            for way, link in (("R", "xp"), ("L", "xm")):
                add((way + "1", j, 0), link, 2 * unit, [S, L], (j + KEYS[2], 1))
                add((way + "1", j, 1), link, 2 * unit, h, (j + KEYS[2], 1))
            far = [("R2", j), ("L2", j)]
            if modes[j] == "b":
                add(far[0], "xp", 2 * unit, [("R1", j, 0)], (j + KEYS[3], 0))
                add(far[1], "xm", 2 * unit, [("L1", j, 1)], (j + KEYS[3], 0))
            else:
                add(far[0], "xp", unit, [("R1", j, 0)], (j + KEYS[3], 0))
                add(far[1], "xm", unit, [("L1", j, 0)], (j + KEYS[3], 0))
                add(("H", j, 2), "zh", 2 * unit, far, j + KEYS[1])
                far = far + [("H", j, 2)]
            got = {0: [S, L] + h, -1: [("R1", j, 0), ("R1", j, 1)], 1: [("L1", j, 0), ("L1", j, 1)], 2: far}
        elif modes[j] == "m":
            add(("H", j, 9), "zh", unit, [L], j + KEYS[0])
            for way, link in (("R", "xp"), ("L", "xm")):
                add((way + "1", j, 0), link, unit, [], (j, 1))
                add((way + "1", j, 1), link, unit, [L], (j, 1))
                add((way + "1", j, 2), link, unit, [("H", j, 9)], (j, 1))
                add((way + "3", j), link, unit // 2, [(way + "1", j, 2)], (j, 0))
            add(("R2", j), "xp", unit, [("R1", j, 0)], (j, 0))
            add(("L2", j), "xm", unit, [("L1", j, 1)], (j, 0))
            for d, dep in ((0, S), (-1, ("R1", j, 0)), (1, ("L1", j, 0)), (2, ("R2", j))):
                add(("H", j, d), "zh", unit, [dep], j + KEYS[1])
            got = {0: [S, L, ("H", j, 9)], -1: [("R1", j, k) for k in range(3)], 1: [("L1", j, k) for k in range(3)],
                   2: [("R2", j), ("L2", j), ("R3", j), ("L3", j)]}
            for d in got:
                got[d] = got[d] + [("H", j, d)]
        else:
            for way, link in (("R", "xp"), ("L", "xm")):
                add((way + "1", j, 0), link, unit, [], (j, 1))
                add((way + "1", j, 1), link, unit, [L], (j, 1))
            add(("R2", j), "xp", unit, [("R1", j, 0)], (j, 0))
            add(("L2", j), "xm", unit, [("L1", j, 1)], (j, 0))
            pre = {0: [S, L], -1: [("R1", j, 0), ("R1", j, 1)], 1: [("L1", j, 0), ("L1", j, 1)], 2: [("R2", j), ("L2", j)]}
            got = {}
            for d in (0, -1, 1, 2):
                add(("H", j, d), "zh", 2 * unit, pre[d], j + KEYS[1])
                got[d] = pre[d] + [("H", j, d)]
        for d in (0, -1, 1, 2):
            add(("D", j, d), "dd", 4 * unit, got[d], j)
            need[j, d] = got[d] + [("D", j, d)]
        add(("Y", j), "zl", unit, [("C", j)], j)
    a_need = {0: [("AS",)], 1: [], -1: [], 2: []}
    for q in range(A_PIECES):
        add(("AL", q), "zl", a_unit, [("AS",)], 0.75 * q)
        for t in (0, 1):
            dep = [("AS",)] if t == 0 else [("AL", q)]
            add(("AR1", t, q), "yp", a_unit, dep, 4 * t + q)
            add(("AL1", t, q), "ym", a_unit, dep, 4 * t + q)
            a_need[-1].append(("AR1", t, q))
            a_need[1].append(("AL1", t, q))
        add(("AR2", q), "yp", a_unit, [("AR1", 0, q)], 8 + q)
        add(("AL2", q), "ym", a_unit, [("AL1", 1, q)], 8 + q)
        a_need[0].append(("AL", q))
        a_need[2] += [("AR2", q), ("AL2", q)]
    a_all = sum(a_need.values(), [])

    tasks = []
    left = []
    for j in range(chunks):
        for e in (0, -1, 1, 2):
            if j < chunks - TAIL_CHUNKS:
                left.append((j, "y", e, sum((need[j, d] for d in (0, -1, 1, 2)), []), a_need[e]))
            else:
                left.append((j, "x", e, need[j, e], a_all))

    prog = []
    t = 0.0
    at = {("AS",): 3.0}
    for j in range(chunks):
        at[("S", j)] = 2.5 + 0.3 * j
    eager = set().union(*(v[2] for v in sends.values()))
    done = set()
    waiting = dict(sends)
    busy = {k: 0.0 for k in RATE}
    out = {k: [] for k in RATE}
    ready_at = {}
    computed = 0
    parts = {}

    def arrived(events, when):
        return all(n in done or at.get(n, 1e9) <= when for n in events)

    def settle(events):
        for n in events:
            if n not in done:
                done.add(n)
                prog.append(("wait", n))

    while True:
        for link in RATE:
            out[link] = [e for e in out[link] if e > t]
            while len(out[link]) < DEPTH_Q:
                ready = [n for n, v in waiting.items() if v[0] == link and v[2] <= done]
                if not ready:
                    break
                name = min(ready, key=lambda n: (waiting[n][3], str(n)))
                size = waiting.pop(name)[1]
                busy[link] = max(busy[link], t + 0.2) + size / RATE[link]
                out[link].append(busy[link])
                at[name] = busy[link] + LAT.get(link, PLAN_LAT)
                prog.append(("start", name))
        now = sorted((v, str(n), n) for n, v in at.items() if n in eager and n not in done and v <= t)
        if now:
            settle([now[0][2]])
            continue
        margin = MARGIN if len(left) > 4 * TAIL_CHUNKS else 0.0
        if len(tasks) - computed < SLOTS:
            pick = [v for v in left if arrived(v[3], t - margin) and arrived(v[4], t - margin)]
            if pick:
                task = pick[0]
                left.remove(task)
                settle(task[3])
                settle(task[4])
                prog.append(("load", len(tasks)))
                ready_at[len(tasks)] = t + 1.7 if task[0] < chunks - 1 else t
                tasks.append(task[:3])
                continue
        if computed < len(tasks) and ready_at[computed] <= t:
            prog.append(("compute", computed))
            j = tasks[computed][0]
            t += block_us
            computed += 1
            parts[j] = parts.get(j, 0) + 1
            if parts[j] == 4:
                done.add(("C", j))
            continue
        later = [v for n, v in at.items() if n in eager and n not in done]
        later += [e for link in RATE for e in out[link] if e > t]
        later += [v for k, v in ready_at.items() if k >= computed]
        later += [v + margin for n, v in at.items() if n not in done and v + margin > t]
        later = [v for v in later if v > t]
        if not later:
            break
        t = min(later)
    if waiting or left or computed < len(tasks):
        raise ValueError("plan stuck")
    return prog, tasks, list(sends), t


def body(prog, tasks, names, modes, dims, a_ref, x_ref, y_ref, xg, av, xv, xt, xs, yv, acc, ssem, rsem, lsem, vsem):
    layout, s, kb, half, kk = dims
    chunks = len(layout)
    z, y, i = lax.axis_index("depth"), lax.axis_index("col"), lax.axis_index("row")
    x, c = i // 2, i % 2
    zh, pi = z // 2, z % 2
    nu = (zh + pi) % 2
    zl_peer = 2 * zh + 1 - pi
    zh_peer = 3 - z

    def xat(d):
        return (x + d + 4) % 4

    def yat(d):
        return (y + d + 4) % 4

    dev = {
        "xp": (z, y, 2 * xat(1) + c),
        "xm": (z, y, 2 * xat(-1) + c),
        "yp": (z, yat(1), i),
        "ym": (z, yat(-1), i),
        "zl": (zl_peer, y, i),
        "zh": (zh_peer, y, i),
        "dd": (z, y, 2 * x + 1 - c),
    }

    def cols(j, part):
        return pl.ds(pl.multiple_of(part * half + layout[j][1], 128), layout[j][2])

    def lane(j):
        return pl.ds(0, layout[j][2])

    def xin(j, part):
        return x_ref.at[layout[j][0], :, cols(j, part)]

    def xgat(j, block, rows):
        if j == chunks - 1:
            return xt.at[block, rows]
        return xg.at[j, block, rows, lane(j)]

    rows_a = s // A_PIECES

    def arow(which, q):
        return pl.ds(pl.multiple_of(which * s + q * rows_a, 16), rows_a)

    def krow(core, first, count):
        return pl.ds(pl.multiple_of((4 * core + first) * s, 16), count * s)

    def yrow(which):
        return pl.ds(pl.multiple_of(which * s, 16), s)

    def ends(name, recv):
        kind = name[0]
        if kind in ("AL", "AR1", "AL1", "AR2", "AL2"):
            q = name[-1]
            if kind == "AL":
                who = 1 - pi if recv else pi
                ref = av.at[y, arow(who, q)]
                return ref, ref, "zl"
            right = kind in ("AR1", "AR2")
            step = (-1 if right else 1) if recv else 0
            if kind in ("AR1", "AL1"):
                who = pi if name[1] == 0 else 1 - pi
                ref = av.at[yat(step), arow(who, q)]
            else:
                who = pi if right else 1 - pi
                ref = av.at[yat(step + (-1 if right else 1)), arow(who, q)]
            return ref, ref, "yp" if right else "ym"
        j = name[1]
        if kind == "L":
            ref = xgat(j, x, krow(c, zl_peer if recv else z, 1))
            return (ref if recv else xin(j, 1 - nu)), ref, "zl"
        if kind == "Y":
            part = 1 - nu if recv else nu
            ref = y_ref.at[layout[j][0], :, cols(j, part)]
            return yv.at[j, :, lane(j)], ref, "zl"
        if kind == "D":
            ref = xgat(j, xat(name[2]), krow(1 - c if recv else c, 0, 4))
            return ref, ref, "dd"
        own, pair, other = krow(c, z, 1), krow(c, 2 * zh, 2), krow(c, 2 * (1 - zh), 2)
        if kind == "H":
            if modes[j] in "bc" and name[2] != 2:
                at = z if name[2] == 0 else zl_peer
                ref = xgat(j, x, krow(c, 3 - at if recv else at, 1))
                return (xin(j, nu) if name[2] == 0 and not recv else ref), ref, "zh"
            if modes[j] == "m":
                at, block = (zl_peer, x) if name[2] == 9 else (z, xat(name[2]))
                ref = xgat(j, block, krow(c, 3 - at if recv else at, 1))
                return ref, ref, "zh"
            ref = xgat(j, xat(name[2]), other if recv else pair)
            return ref, ref, "zh"
        right = kind[0] == "R"
        link = "xp" if right else "xm"
        step = (-1 if right else 1) if recv else 0
        if modes[j] == "b" or (modes[j] == "c" and kind[1] == "1"):
            parts = (pair, other)
        else:
            parts = (own, krow(c, zl_peer, 1), krow(c, 3 - zl_peer, 1))
        if kind[1] == "3":
            at = (4 * c + 3 - zl_peer) * s + (0 if right else s // 2)
            ref = xgat(j, xat(step + (-1 if right else 1)), pl.ds(pl.multiple_of(at, 16), s // 2))
            return ref, ref, link
        if kind[1] == "1":
            ref = xgat(j, xat(step), parts[name[2]])
            direct = modes[j] in "am" and name[2] == 0 and not recv
            return (xin(j, nu) if direct else ref), ref, link
        ref = xgat(j, xat(step + (-1 if right else 1)), parts[0 if right else 1])
        return ref, ref, link

    index = {n: k for k, n in enumerate(names)}

    def remote(name, recv=False):
        src, dst, link = ends(name, recv)
        return pltpu.make_async_remote_copy(
            src_ref=src, dst_ref=dst, send_sem=ssem.at[index[name]], recv_sem=rsem.at[index[name]],
            device_id=dev[link], device_id_type=MESH)

    def stage_in(j):
        dst = xgat(j, x, krow(c, z, 1)) if j == chunks - 1 else xs.at[j, :, lane(j)]
        return pltpu.make_async_copy(xin(j, nu), dst, lsem.at[j])

    def stage_out(j):
        return pltpu.make_async_copy(xs.at[j, :, lane(j)], xgat(j, x, krow(c, z, 1)), lsem.at[chunks + j])

    def a_in():
        return pltpu.make_async_copy(a_ref, av.at[y, yrow(pi)], lsem.at[2 * chunks])

    def load(task):
        j, axis, e = tasks[task]
        slot = task % SLOTS
        block = yat(e) if axis == "y" else xat(e)
        return pltpu.make_async_copy(xgat(j, block, pl.ds(0, kb)), xv.at[slot, :, lane(j)], vsem.at[slot])

    barrier = pltpu.get_barrier_semaphore()
    for peer in dev.values():
        pl.semaphore_signal(barrier, inc=1, device_id=peer, device_id_type=MESH)
    for j in range(chunks):
        stage_in(j).start()
    a_in().start()
    pl.semaphore_wait(barrier, len(dev))

    staged = [False]

    def finish_stage():
        for j in range(chunks - 1):
            stage_in(j).wait()
            stage_out(j).start()
        staged[0] = True

    received = set()
    parts = [0] * chunks
    for op, what in prog:
        if op == "start":
            if what != ("Y", tasks[-1][0]):
                remote(what).start()
        elif op == "load":
            if tasks[what][0] < chunks - 1:
                load(what).start()
        elif op == "wait":
            if not staged[0]:
                finish_stage()
            if what[0] == "S":
                (stage_in if what[1] == chunks - 1 else stage_out)(what[1]).wait()
            elif what[0] == "AS":
                a_in().wait()
            else:
                remote(what, True).wait_recv()
                received.add(what)
        else:
            j, axis, e = tasks[what]
            slot = what % SLOTS
            wide = lane(j)
            if j < chunks - 1:
                load(what).wait()
            if parts[j] == 0:
                acc[j, :, wide] = jnp.zeros((2 * s, layout[j][2]), jnp.float32)
            block = yat(e) if axis == "y" else xat(e)

            def rhs(lanes, slot=slot, block=block, j=j, wide=wide):
                return xt[block, lanes, :] if j == chunks - 1 else xv[slot, lanes, wide]

            whole = what == len(tasks) - 1 or (what >= len(tasks) - WHOLE_K and layout[j][2] == 256)
            deep = kb if whole else kk

            def step(k, rows, rhs=rhs, block=block, j=j, wide=wide, deep=deep):
                lanes = slice(None) if deep == kb else pl.ds(pl.multiple_of(k * deep, 128), deep)
                acc[j, rows, wide] += jnp.dot(av[block, rows, lanes], rhs(lanes), preferred_element_type=jnp.float32)

            def loop(rows, step=step, deep=deep):
                if deep == kb:
                    step(0, rows)
                else:
                    lax.fori_loop(0, kb // deep, lambda k, carry: (step(k, rows), carry)[1], 0)

            parts[j] += 1
            if what == len(tasks) - 1:
                loop(yrow(1 - pi))
                yv[j, :, wide] = acc[j, yrow(1 - pi), wide].astype(yv.dtype)
                remote(("Y", j)).start()
                loop(yrow(pi))
                y_ref[layout[j][0], :, cols(j, nu)] = acc[j, yrow(pi), wide].astype(y_ref.dtype)
                continue
            loop(slice(None))
            if parts[j] == 4:
                yv[j, :, wide] = acc[j, yrow(1 - pi), wide].astype(yv.dtype)
                y_ref[layout[j][0], :, cols(j, nu)] = acc[j, yrow(pi), wide].astype(y_ref.dtype)

    for name in names:
        if name not in received:
            remote(name, True).wait_recv()
    for name in names:
        remote(name).wait_send()


def solution(mesh):
    def local(a, x):
        rhs, s, xc = x.shape
        kb = a.shape[1]
        half = xc // 2
        width = 256 if half % 256 == 0 else 128
        layout = [(r, at, width) for r in range(rhs) for at in range(0, half, width)]
        if width == 256:
            r, at, _ = layout.pop()
            layout += [(r, at, 128), (r, at + 128, 128)]
        chunks = len(layout)
        modes = (MODES * chunks)[:chunks]
        kk = 1024 if kb % 1024 == 0 else 256
        units = [2 * s * w for _, _, w in layout]
        prog, tasks, names, _ = make_plan(units, modes, 2 * s * kb // A_PIECES, BLOCK_US)
        dims = (layout, s, kb, half, kk)
        any_spec = pl.BlockSpec(memory_space=pl.ANY)
        y, _ = pl.pallas_call(
            functools.partial(body, prog, tasks, names, modes, dims),
            out_shape=(pltpu.VMEM(x.shape, x.dtype), jax.ShapeDtypeStruct((chunks, 4, kb, width), x.dtype)),
            in_specs=[any_spec, any_spec],
            out_specs=(pl.BlockSpec(memory_space=pltpu.VMEM), any_spec),
            scratch_shapes=[
                pltpu.VMEM((4, 2 * s, kb), a.dtype),
                pltpu.VMEM((SLOTS, kb, width), x.dtype),
                pltpu.VMEM((4, kb, layout[-1][2]), x.dtype),
                pltpu.VMEM((chunks, s, width), x.dtype),
                pltpu.VMEM((chunks, s, width), x.dtype),
                pltpu.VMEM((chunks, 2 * s, width), jnp.float32),
                pltpu.SemaphoreType.DMA((len(names),)),
                pltpu.SemaphoreType.DMA((len(names),)),
                pltpu.SemaphoreType.DMA((2 * chunks + 1,)),
                pltpu.SemaphoreType.DMA((SLOTS,)),
            ],
            compiler_params=pltpu.CompilerParams(collective_id=0, has_side_effects=True, vmem_limit_bytes=54 * 1024 * 1024),
        )(a, x)
        return y

    spec_a = P(("row", "depth"), "col")
    spec_x = P(None, ("row", "depth"), "col")
    return jax.shard_map(local, mesh=mesh, in_specs=(spec_a, spec_x), out_specs=spec_x, check_vma=False)
```

```python
import functools

import jax
import jax.numpy as jnp
from jax import lax
from jax.experimental import pallas as pl
from jax.experimental.pallas import tpu as pltpu
from jax.sharding import PartitionSpec as P

MESH = pl.DeviceIdType.MESH
MODES = "abbababmabacbb"
A_PIECES = 4
SLOTS = 5
DEPTH_Q = 3
TAIL_CHUNKS = 6
MARGIN = 0.5
PLAN_LAT = 4.5
BLOCK_US = 1.6
RATE = {"xp": 46.0e3, "xm": 46.0e3, "yp": 46.0e3, "ym": 46.0e3, "zl": 46.0e3, "zh": 46.0e3, "dd": 300.0e3}
LAT = {"dd": 2.5}
NEAR = 2
KEYS = (-9.0, -1.5, 0.6, 1.2)


def make_plan(units, modes, a_unit, block_us):
    sends = {}
    chunks = len(units)

    def add(name, link, size, deps, key):
        sends[name] = (link, size, frozenset(deps), key)

    need = {}
    for j in range(chunks):
        S, L, unit = ("S", j), ("L", j), units[j]
        add(L, "zl", unit, [], j - 1)
        if modes[j] in "bc":
            add(("H", j, 0), "zh", unit, [], j + KEYS[0])
            add(("H", j, 1), "zh", unit, [L], j + KEYS[0])
            h = [("H", j, 0), ("H", j, 1)]
            for way, link in (("R", "xp"), ("L", "xm")):
                add((way + "1", j, 0), link, 2 * unit, [S, L], (j + KEYS[2], 1))
                add((way + "1", j, 1), link, 2 * unit, h, (j + KEYS[2], 1))
            far = [("R2", j), ("L2", j)]
            if modes[j] == "b":
                add(far[0], "xp", 2 * unit, [("R1", j, 0)], (j + KEYS[3], 0))
                add(far[1], "xm", 2 * unit, [("L1", j, 1)], (j + KEYS[3], 0))
            else:
                add(far[0], "xp", unit, [("R1", j, 0)], (j + KEYS[3], 0))
                add(far[1], "xm", unit, [("L1", j, 0)], (j + KEYS[3], 0))
                add(("H", j, 2), "zh", 2 * unit, far, j + KEYS[1])
                far = far + [("H", j, 2)]
            got = {0: [S, L] + h, -1: [("R1", j, 0), ("R1", j, 1)], 1: [("L1", j, 0), ("L1", j, 1)], 2: far}
        elif modes[j] == "m":
            add(("H", j, 9), "zh", unit, [L], j + KEYS[0])
            for way, link in (("R", "xp"), ("L", "xm")):
                add((way + "1", j, 0), link, unit, [], (j, 1))
                add((way + "1", j, 1), link, unit, [L], (j, 1))
                add((way + "1", j, 2), link, unit, [("H", j, 9)], (j, 1))
                add((way + "3", j), link, unit // 2, [(way + "1", j, 2)], (j, 0))
            add(("R2", j), "xp", unit, [("R1", j, 0)], (j, 0))
            add(("L2", j), "xm", unit, [("L1", j, 1)], (j, 0))
            for d, dep in ((0, S), (-1, ("R1", j, 0)), (1, ("L1", j, 0)), (2, ("R2", j))):
                add(("H", j, d), "zh", unit, [dep], j + KEYS[1])
            got = {0: [S, L, ("H", j, 9)], -1: [("R1", j, k) for k in range(3)], 1: [("L1", j, k) for k in range(3)],
                   2: [("R2", j), ("L2", j), ("R3", j), ("L3", j)]}
            for d in got:
                got[d] = got[d] + [("H", j, d)]
        else:
            for way, link in (("R", "xp"), ("L", "xm")):
                add((way + "1", j, 0), link, unit, [], (j, 1))
                add((way + "1", j, 1), link, unit, [L], (j, 1))
            add(("R2", j), "xp", unit, [("R1", j, 0)], (j, 0))
            add(("L2", j), "xm", unit, [("L1", j, 1)], (j, 0))
            pre = {0: [S, L], -1: [("R1", j, 0), ("R1", j, 1)], 1: [("L1", j, 0), ("L1", j, 1)], 2: [("R2", j), ("L2", j)]}
            got = {}
            for d in (0, -1, 1, 2):
                add(("H", j, d), "zh", 2 * unit, pre[d], j + KEYS[1])
                got[d] = pre[d] + [("H", j, d)]
        for d in (0, -1, 1, 2):
            add(("D", j, d), "dd", 4 * unit, got[d], j)
            need[j, d] = got[d] + [("D", j, d)]
        add(("Y", j), "zl", unit, [("C", j)], j)
    a_need = {0: [("AS",)], 1: [], -1: [], 2: []}
    for q in range(A_PIECES):
        add(("AL", q), "zl", a_unit, [("AS",)], 0.75 * q)
        for t in (0, 1):
            dep = [("AS",)] if t == 0 else [("AL", q)]
            add(("AR1", t, q), "yp", a_unit, dep, 4 * t + q)
            add(("AL1", t, q), "ym", a_unit, dep, 4 * t + q)
            a_need[-1].append(("AR1", t, q))
            a_need[1].append(("AL1", t, q))
        add(("AR2", q), "yp", a_unit, [("AR1", 0, q)], 8 + q)
        add(("AL2", q), "ym", a_unit, [("AL1", 1, q)], 8 + q)
        a_need[0].append(("AL", q))
        a_need[2] += [("AR2", q), ("AL2", q)]
    a_all = sum(a_need.values(), [])

    tasks = []
    left = []
    for j in range(chunks):
        for e in (0, -1, 1, 2):
            if j < chunks - TAIL_CHUNKS:
                left.append((j, "y", e, sum((need[j, d] for d in (0, -1, 1, 2)), []), a_need[e]))
            else:
                left.append((j, "x", e, need[j, e], a_all))

    prog = []
    t = 0.0
    at = {("AS",): 3.0}
    for j in range(chunks):
        at[("S", j)] = 2.5 + 0.3 * j
    eager = set().union(*(v[2] for v in sends.values()))
    done = set()
    waiting = dict(sends)
    busy = {k: 0.0 for k in RATE}
    out = {k: [] for k in RATE}
    ready_at = {}
    computed = 0
    parts = {}

    def arrived(events, when):
        return all(n in done or at.get(n, 1e9) <= when for n in events)

    def settle(events):
        for n in events:
            if n not in done:
                done.add(n)
                prog.append(("wait", n))

    while True:
        for link in RATE:
            out[link] = [e for e in out[link] if e > t]
            while len(out[link]) < DEPTH_Q:
                ready = [n for n, v in waiting.items() if v[0] == link and v[2] <= done]
                if not ready:
                    break
                name = min(ready, key=lambda n: (waiting[n][3], str(n)))
                size = waiting.pop(name)[1]
                busy[link] = max(busy[link], t + 0.2) + size / RATE[link]
                out[link].append(busy[link])
                at[name] = busy[link] + LAT.get(link, PLAN_LAT)
                prog.append(("start", name))
        now = sorted((v, str(n), n) for n, v in at.items() if n in eager and n not in done and v <= t)
        if now:
            settle([now[0][2]])
            continue
        margin = MARGIN if len(left) > 4 * TAIL_CHUNKS else 0.0
        if len(tasks) - computed < SLOTS:
            pick = [v for v in left if arrived(v[3], t - margin) and arrived(v[4], t - margin)]
            if pick:
                task = pick[0]
                left.remove(task)
                settle(task[3])
                settle(task[4])
                prog.append(("load", len(tasks)))
                ready_at[len(tasks)] = t + 1.7 if task[0] < chunks - NEAR else t
                tasks.append(task[:3])
                continue
        if computed < len(tasks) and ready_at[computed] <= t:
            prog.append(("compute", computed))
            j = tasks[computed][0]
            t += block_us
            computed += 1
            parts[j] = parts.get(j, 0) + 1
            if parts[j] == 4:
                done.add(("C", j))
            continue
        later = [v for n, v in at.items() if n in eager and n not in done]
        later += [e for link in RATE for e in out[link] if e > t]
        later += [v for k, v in ready_at.items() if k >= computed]
        later += [v + margin for n, v in at.items() if n not in done and v + margin > t]
        later = [v for v in later if v > t]
        if not later:
            break
        t = min(later)
    if waiting or left or computed < len(tasks):
        raise ValueError("plan stuck")
    return prog, tasks, list(sends), t


def body(prog, tasks, names, modes, dims, a_ref, x_ref, y_ref, xg, av, xv, xt, xs, yv, acc, ssem, rsem, lsem, vsem):
    layout, s, kb, half, kk = dims
    chunks = len(layout)
    near = chunks - NEAR
    z, y, i = lax.axis_index("depth"), lax.axis_index("col"), lax.axis_index("row")
    x, c = i // 2, i % 2
    zh, pi = z // 2, z % 2
    nu = (zh + pi) % 2
    zl_peer = 2 * zh + 1 - pi
    zh_peer = 3 - z

    def xat(d):
        return (x + d + 4) % 4

    def yat(d):
        return (y + d + 4) % 4

    dev = {
        "xp": (z, y, 2 * xat(1) + c),
        "xm": (z, y, 2 * xat(-1) + c),
        "yp": (z, yat(1), i),
        "ym": (z, yat(-1), i),
        "zl": (zl_peer, y, i),
        "zh": (zh_peer, y, i),
        "dd": (z, y, 2 * x + 1 - c),
    }

    def cols(j, part):
        return pl.ds(pl.multiple_of(part * half + layout[j][1], 128), layout[j][2])

    def lane(j):
        return pl.ds(0, layout[j][2])

    def xin(j, part):
        return x_ref.at[layout[j][0], :, cols(j, part)]

    def xgat(j, block, rows):
        if j >= near:
            return xt.at[j - near, block, rows]
        return xg.at[j, block, rows, lane(j)]

    rows_a = s // A_PIECES

    def arow(which, q):
        return pl.ds(pl.multiple_of(which * s + q * rows_a, 16), rows_a)

    def krow(core, first, count):
        return pl.ds(pl.multiple_of((4 * core + first) * s, 16), count * s)

    def yrow(which):
        return pl.ds(pl.multiple_of(which * s, 16), s)

    def ends(name, recv):
        kind = name[0]
        if kind in ("AL", "AR1", "AL1", "AR2", "AL2"):
            q = name[-1]
            if kind == "AL":
                who = 1 - pi if recv else pi
                ref = av.at[y, arow(who, q)]
                return ref, ref, "zl"
            right = kind in ("AR1", "AR2")
            step = (-1 if right else 1) if recv else 0
            if kind in ("AR1", "AL1"):
                who = pi if name[1] == 0 else 1 - pi
                ref = av.at[yat(step), arow(who, q)]
            else:
                who = pi if right else 1 - pi
                ref = av.at[yat(step + (-1 if right else 1)), arow(who, q)]
            return ref, ref, "yp" if right else "ym"
        j = name[1]
        if kind == "L":
            ref = xgat(j, x, krow(c, zl_peer if recv else z, 1))
            return (ref if recv else xin(j, 1 - nu)), ref, "zl"
        if kind == "Y":
            part = 1 - nu if recv else nu
            ref = y_ref.at[layout[j][0], :, cols(j, part)]
            return yv.at[j, :, lane(j)], ref, "zl"
        if kind == "D":
            ref = xgat(j, xat(name[2]), krow(1 - c if recv else c, 0, 4))
            return ref, ref, "dd"
        own, pair, other = krow(c, z, 1), krow(c, 2 * zh, 2), krow(c, 2 * (1 - zh), 2)
        if kind == "H":
            if modes[j] in "bc" and name[2] != 2:
                at = z if name[2] == 0 else zl_peer
                ref = xgat(j, x, krow(c, 3 - at if recv else at, 1))
                return (xin(j, nu) if name[2] == 0 and not recv else ref), ref, "zh"
            if modes[j] == "m":
                at, block = (zl_peer, x) if name[2] == 9 else (z, xat(name[2]))
                ref = xgat(j, block, krow(c, 3 - at if recv else at, 1))
                return ref, ref, "zh"
            ref = xgat(j, xat(name[2]), other if recv else pair)
            return ref, ref, "zh"
        right = kind[0] == "R"
        link = "xp" if right else "xm"
        step = (-1 if right else 1) if recv else 0
        if modes[j] == "b" or (modes[j] == "c" and kind[1] == "1"):
            parts = (pair, other)
        else:
            parts = (own, krow(c, zl_peer, 1), krow(c, 3 - zl_peer, 1))
        if kind[1] == "3":
            at = (4 * c + 3 - zl_peer) * s + (0 if right else s // 2)
            ref = xgat(j, xat(step + (-1 if right else 1)), pl.ds(pl.multiple_of(at, 16), s // 2))
            return ref, ref, link
        if kind[1] == "1":
            ref = xgat(j, xat(step), parts[name[2]])
            direct = modes[j] in "am" and name[2] == 0 and not recv
            return (xin(j, nu) if direct else ref), ref, link
        ref = xgat(j, xat(step + (-1 if right else 1)), parts[0 if right else 1])
        return ref, ref, link

    index = {n: k for k, n in enumerate(names)}

    def remote(name, recv=False):
        src, dst, link = ends(name, recv)
        return pltpu.make_async_remote_copy(
            src_ref=src, dst_ref=dst, send_sem=ssem.at[index[name]], recv_sem=rsem.at[index[name]],
            device_id=dev[link], device_id_type=MESH)

    def stage_in(j):
        dst = xgat(j, x, krow(c, z, 1)) if j >= near else xs.at[j, :, lane(j)]
        return pltpu.make_async_copy(xin(j, nu), dst, lsem.at[j])

    def stage_out(j):
        return pltpu.make_async_copy(xs.at[j, :, lane(j)], xgat(j, x, krow(c, z, 1)), lsem.at[chunks + j])

    def a_in():
        return pltpu.make_async_copy(a_ref, av.at[y, yrow(pi)], lsem.at[2 * chunks])

    def load(task):
        j, axis, e = tasks[task]
        slot = task % SLOTS
        block = yat(e) if axis == "y" else xat(e)
        return pltpu.make_async_copy(xgat(j, block, pl.ds(0, kb)), xv.at[slot, :, lane(j)], vsem.at[slot])

    barrier = pltpu.get_barrier_semaphore()
    for peer in dev.values():
        pl.semaphore_signal(barrier, inc=1, device_id=peer, device_id_type=MESH)
    for j in range(chunks):
        stage_in(j).start()
    a_in().start()
    pl.semaphore_wait(barrier, len(dev))

    staged = [False]

    def finish_stage():
        for j in range(near):
            stage_in(j).wait()
            stage_out(j).start()
        staged[0] = True

    received = set()
    parts = [0] * chunks
    for op, what in prog:
        if op == "start":
            remote(what).start()
        elif op == "load":
            if tasks[what][0] < near:
                load(what).start()
        elif op == "wait":
            if not staged[0]:
                finish_stage()
            if what[0] == "S":
                (stage_in if what[1] >= near else stage_out)(what[1]).wait()
            elif what[0] == "AS":
                a_in().wait()
            else:
                remote(what, True).wait_recv()
                received.add(what)
        else:
            j, axis, e = tasks[what]
            slot = what % SLOTS
            wide = lane(j)
            if j < near:
                load(what).wait()
            if parts[j] == 0:
                acc[j, :, wide] = jnp.zeros((2 * s, layout[j][2]), jnp.float32)
            block = yat(e) if axis == "y" else xat(e)

            def rhs(lanes, slot=slot, block=block, j=j, wide=wide):
                return xt[j - near, block, lanes, :] if j >= near else xv[slot, lanes, wide]

            def step(k, carry, rhs=rhs, block=block, j=j, wide=wide):
                lanes = pl.ds(pl.multiple_of(k * kk, 128), kk)
                acc[j, :, wide] += jnp.dot(av[block, :, lanes], rhs(lanes), preferred_element_type=jnp.float32)
                return carry

            lax.fori_loop(0, kb // kk, step, 0)
            parts[j] += 1
            if parts[j] == 4:
                yv[j, :, wide] = acc[j, yrow(1 - pi), wide].astype(yv.dtype)
                y_ref[layout[j][0], :, cols(j, nu)] = acc[j, yrow(pi), wide].astype(y_ref.dtype)

    for name in names:
        if name not in received:
            remote(name, True).wait_recv()
    for name in names:
        remote(name).wait_send()


def solution(mesh):
    def local(a, x):
        rhs, s, xc = x.shape
        kb = a.shape[1]
        half = xc // 2
        width = 256 if half % 256 == 0 else 128
        layout = [(r, at, width) for r in range(rhs) for at in range(0, half, width)]
        if width == 256:
            split = layout[-2:]
            layout = layout[:-2] + [(r, at + more, 128) for r, at, _ in split for more in (0, 128)]
        chunks = len(layout)
        modes = (MODES * chunks)[:chunks]
        kk = 1024 if kb % 1024 == 0 else 256
        units = [2 * s * w for _, _, w in layout]
        prog, tasks, names, _ = make_plan(units, modes, 2 * s * kb // A_PIECES, BLOCK_US)
        dims = (layout, s, kb, half, kk)
        any_spec = pl.BlockSpec(memory_space=pl.ANY)
        y, _ = pl.pallas_call(
            functools.partial(body, prog, tasks, names, modes, dims),
            out_shape=(pltpu.VMEM(x.shape, x.dtype), jax.ShapeDtypeStruct((chunks, 4, kb, width), x.dtype)),
            in_specs=[any_spec, any_spec],
            out_specs=(pl.BlockSpec(memory_space=pltpu.VMEM), any_spec),
            scratch_shapes=[
                pltpu.VMEM((4, 2 * s, kb), a.dtype),
                pltpu.VMEM((SLOTS, kb, width), x.dtype),
                pltpu.VMEM((NEAR, 4, kb, layout[-1][2]), x.dtype),
                pltpu.VMEM((chunks, s, width), x.dtype),
                pltpu.VMEM((chunks, s, width), x.dtype),
                pltpu.VMEM((chunks, 2 * s, width), jnp.float32),
                pltpu.SemaphoreType.DMA((len(names),)),
                pltpu.SemaphoreType.DMA((len(names),)),
                pltpu.SemaphoreType.DMA((2 * chunks + 1,)),
                pltpu.SemaphoreType.DMA((SLOTS,)),
            ],
            compiler_params=pltpu.CompilerParams(collective_id=0, has_side_effects=True, vmem_limit_bytes=54 * 1024 * 1024),
        )(a, x)
        return y

    spec_a = P(("row", "depth"), "col")
    spec_x = P(None, ("row", "depth"), "col")
    return jax.shard_map(local, mesh=mesh, in_specs=(spec_a, spec_x), out_specs=spec_x, check_vma=False)
```

```python
import functools

import jax
import jax.numpy as jnp
from jax import lax
from jax.experimental import pallas as pl
from jax.experimental.pallas import tpu as pltpu
from jax.sharding import PartitionSpec as P

MESH = pl.DeviceIdType.MESH
MODES = "abbmbaababacbb"
A_PIECES = 4
SLOTS = 5
DEPTH_Q = 3
TAIL_CHUNKS = 5
MARGIN = 2.0
PLAN_LAT = 5.0
BLOCK_US = 1.6
RATE = {"xp": 46.0e3, "xm": 46.0e3, "yp": 46.0e3, "ym": 46.0e3, "zl": 46.0e3, "zh": 46.0e3, "dd": 300.0e3}
LAT = {"dd": 2.5}
NEAR = 2
KEYS = (-3.0, 1.5, 0.6, 1.2)


def make_plan(units, modes, a_unit, block_us):
    sends = {}
    chunks = len(units)

    def add(name, link, size, deps, key):
        sends[name] = (link, size, frozenset(deps), key)

    need = {}
    for j in range(chunks):
        S, L, unit = ("S", j), ("L", j), units[j]
        add(L, "zl", unit, [], j - 1)
        if modes[j] in "bc":
            add(("H", j, 0), "zh", unit, [], j + KEYS[0])
            add(("H", j, 1), "zh", unit, [L], j + KEYS[0])
            h = [("H", j, 0), ("H", j, 1)]
            for way, link in (("R", "xp"), ("L", "xm")):
                add((way + "1", j, 0), link, 2 * unit, [S, L], (j + KEYS[2], 1))
                add((way + "1", j, 1), link, 2 * unit, h, (j + KEYS[2], 1))
            far = [("R2", j), ("L2", j)]
            if modes[j] == "b":
                add(far[0], "xp", 2 * unit, [("R1", j, 0)], (j + KEYS[3], 0))
                add(far[1], "xm", 2 * unit, [("L1", j, 1)], (j + KEYS[3], 0))
            else:
                add(far[0], "xp", unit, [("R1", j, 0)], (j + KEYS[3], 0))
                add(far[1], "xm", unit, [("L1", j, 0)], (j + KEYS[3], 0))
                add(("H", j, 2), "zh", 2 * unit, far, j + KEYS[1])
                far = far + [("H", j, 2)]
            got = {0: [S, L] + h, -1: [("R1", j, 0), ("R1", j, 1)], 1: [("L1", j, 0), ("L1", j, 1)], 2: far}
        elif modes[j] == "m":
            add(("H", j, 9), "zh", unit, [L], j + KEYS[0])
            for way, link in (("R", "xp"), ("L", "xm")):
                add((way + "1", j, 0), link, unit, [], (j, 1))
                add((way + "1", j, 1), link, unit, [L], (j, 1))
                add((way + "1", j, 2), link, unit, [("H", j, 9)], (j, 1))
                add((way + "3", j), link, unit // 2, [(way + "1", j, 2)], (j, 0))
            add(("R2", j), "xp", unit, [("R1", j, 0)], (j, 0))
            add(("L2", j), "xm", unit, [("L1", j, 1)], (j, 0))
            for d, dep in ((0, S), (-1, ("R1", j, 0)), (1, ("L1", j, 0)), (2, ("R2", j))):
                add(("H", j, d), "zh", unit, [dep], j + KEYS[1])
            got = {0: [S, L, ("H", j, 9)], -1: [("R1", j, k) for k in range(3)], 1: [("L1", j, k) for k in range(3)],
                   2: [("R2", j), ("L2", j), ("R3", j), ("L3", j)]}
            for d in got:
                got[d] = got[d] + [("H", j, d)]
        else:
            for way, link in (("R", "xp"), ("L", "xm")):
                add((way + "1", j, 0), link, unit, [], (j, 1))
                add((way + "1", j, 1), link, unit, [L], (j, 1))
            add(("R2", j), "xp", unit, [("R1", j, 0)], (j, 0))
            add(("L2", j), "xm", unit, [("L1", j, 1)], (j, 0))
            pre = {0: [S, L], -1: [("R1", j, 0), ("R1", j, 1)], 1: [("L1", j, 0), ("L1", j, 1)], 2: [("R2", j), ("L2", j)]}
            got = {}
            for d in (0, -1, 1, 2):
                add(("H", j, d), "zh", 2 * unit, pre[d], j + KEYS[1])
                got[d] = pre[d] + [("H", j, d)]
        for d in (0, -1, 1, 2):
            add(("D", j, d), "dd", 4 * unit, got[d], j)
            need[j, d] = got[d] + [("D", j, d)]
        add(("Y", j), "zl", unit, [("C", j)], j)
    a_need = {0: [("AS",)], 1: [], -1: [], 2: []}
    for q in range(A_PIECES):
        add(("AL", q), "zl", a_unit, [("AS",)], 0.75 * q)
        for t in (0, 1):
            dep = [("AS",)] if t == 0 else [("AL", q)]
            add(("AR1", t, q), "yp", a_unit, dep, 4 * t + q)
            add(("AL1", t, q), "ym", a_unit, dep, 4 * t + q)
            a_need[-1].append(("AR1", t, q))
            a_need[1].append(("AL1", t, q))
        add(("AR2", q), "yp", a_unit, [("AR1", 0, q)], 8 + q)
        add(("AL2", q), "ym", a_unit, [("AL1", 1, q)], 8 + q)
        a_need[0].append(("AL", q))
        a_need[2] += [("AR2", q), ("AL2", q)]
    a_all = sum(a_need.values(), [])

    tasks = []
    left = []
    for j in range(chunks):
        for e in (0, -1, 1, 2):
            if j < chunks - TAIL_CHUNKS:
                left.append((j, "y", e, sum((need[j, d] for d in (0, -1, 1, 2)), []), a_need[e]))
            else:
                left.append((j, "x", e, need[j, e], a_all))

    prog = []
    t = 0.0
    at = {("AS",): 3.0}
    for j in range(chunks):
        at[("S", j)] = 2.5 + 0.3 * j
    eager = set().union(*(v[2] for v in sends.values()))
    done = set()
    waiting = dict(sends)
    busy = {k: 0.0 for k in RATE}
    out = {k: [] for k in RATE}
    ready_at = {}
    computed = 0
    parts = {}

    def arrived(events, when):
        return all(n in done or at.get(n, 1e9) <= when for n in events)

    def settle(events):
        for n in events:
            if n not in done:
                done.add(n)
                prog.append(("wait", n))

    while True:
        for link in RATE:
            out[link] = [e for e in out[link] if e > t]
            while len(out[link]) < DEPTH_Q:
                ready = [n for n, v in waiting.items() if v[0] == link and v[2] <= done]
                if not ready:
                    break
                name = min(ready, key=lambda n: (waiting[n][3], str(n)))
                size = waiting.pop(name)[1]
                busy[link] = max(busy[link], t + 0.2) + size / RATE[link]
                out[link].append(busy[link])
                at[name] = busy[link] + LAT.get(link, PLAN_LAT)
                prog.append(("start", name))
        now = sorted((v, str(n), n) for n, v in at.items() if n in eager and n not in done and v <= t)
        if now:
            settle([now[0][2]])
            continue
        margin = MARGIN if len(left) > 4 * TAIL_CHUNKS else 0.0
        if len(tasks) - computed < SLOTS:
            pick = [v for v in left if arrived(v[3], t - margin) and arrived(v[4], t - margin)]
            if pick:
                task = pick[0]
                left.remove(task)
                settle(task[3])
                settle(task[4])
                prog.append(("load", len(tasks)))
                ready_at[len(tasks)] = t + 1.7 if task[0] < chunks - NEAR else t
                tasks.append(task[:3])
                continue
        if computed < len(tasks) and ready_at[computed] <= t:
            prog.append(("compute", computed))
            j = tasks[computed][0]
            t += block_us
            computed += 1
            parts[j] = parts.get(j, 0) + 1
            if parts[j] == 4:
                done.add(("C", j))
            continue
        later = [v for n, v in at.items() if n in eager and n not in done]
        later += [e for link in RATE for e in out[link] if e > t]
        later += [v for k, v in ready_at.items() if k >= computed]
        later += [v + margin for n, v in at.items() if n not in done and v + margin > t]
        later = [v for v in later if v > t]
        if not later:
            break
        t = min(later)
    if waiting or left or computed < len(tasks):
        raise ValueError("plan stuck")
    return prog, tasks, list(sends), t


def body(prog, tasks, names, modes, dims, a_ref, x_ref, y_ref, xg, av, xv, xt, xs, yv, acc, ssem, rsem, lsem, vsem):
    layout, s, kb, half, kk = dims
    chunks = len(layout)
    near = chunks - NEAR
    z, y, i = lax.axis_index("depth"), lax.axis_index("col"), lax.axis_index("row")
    x, c = i // 2, i % 2
    zh, pi = z // 2, z % 2
    nu = (zh + pi) % 2
    zl_peer = 2 * zh + 1 - pi
    zh_peer = 3 - z

    def xat(d):
        return (x + d + 4) % 4

    def yat(d):
        return (y + d + 4) % 4

    dev = {
        "xp": (z, y, 2 * xat(1) + c),
        "xm": (z, y, 2 * xat(-1) + c),
        "yp": (z, yat(1), i),
        "ym": (z, yat(-1), i),
        "zl": (zl_peer, y, i),
        "zh": (zh_peer, y, i),
        "dd": (z, y, 2 * x + 1 - c),
    }

    def cols(j, part):
        return pl.ds(pl.multiple_of(part * half + layout[j][1], 128), layout[j][2])

    def lane(j):
        return pl.ds(0, layout[j][2])

    def xin(j, part):
        return x_ref.at[layout[j][0], :, cols(j, part)]

    def xgat(j, block, rows):
        if j >= near:
            return xt.at[j - near, block, rows]
        return xg.at[j, block, rows, lane(j)]

    rows_a = s // A_PIECES

    def arow(which, q):
        return pl.ds(pl.multiple_of(which * s + q * rows_a, 16), rows_a)

    def krow(core, first, count):
        return pl.ds(pl.multiple_of((4 * core + first) * s, 16), count * s)

    def yrow(which):
        return pl.ds(pl.multiple_of(which * s, 16), s)

    def ends(name, recv):
        kind = name[0]
        if kind in ("AL", "AR1", "AL1", "AR2", "AL2"):
            q = name[-1]
            if kind == "AL":
                who = 1 - pi if recv else pi
                ref = av.at[y, arow(who, q)]
                return ref, ref, "zl"
            right = kind in ("AR1", "AR2")
            step = (-1 if right else 1) if recv else 0
            if kind in ("AR1", "AL1"):
                who = pi if name[1] == 0 else 1 - pi
                ref = av.at[yat(step), arow(who, q)]
            else:
                who = pi if right else 1 - pi
                ref = av.at[yat(step + (-1 if right else 1)), arow(who, q)]
            return ref, ref, "yp" if right else "ym"
        j = name[1]
        if kind == "L":
            ref = xgat(j, x, krow(c, zl_peer if recv else z, 1))
            return (ref if recv else xin(j, 1 - nu)), ref, "zl"
        if kind == "Y":
            part = 1 - nu if recv else nu
            ref = y_ref.at[layout[j][0], :, cols(j, part)]
            return yv.at[j, :, lane(j)], ref, "zl"
        if kind == "D":
            ref = xgat(j, xat(name[2]), krow(1 - c if recv else c, 0, 4))
            return ref, ref, "dd"
        own, pair, other = krow(c, z, 1), krow(c, 2 * zh, 2), krow(c, 2 * (1 - zh), 2)
        if kind == "H":
            if modes[j] in "bc" and name[2] != 2:
                at = z if name[2] == 0 else zl_peer
                ref = xgat(j, x, krow(c, 3 - at if recv else at, 1))
                return (xin(j, nu) if name[2] == 0 and not recv else ref), ref, "zh"
            if modes[j] == "m":
                at, block = (zl_peer, x) if name[2] == 9 else (z, xat(name[2]))
                ref = xgat(j, block, krow(c, 3 - at if recv else at, 1))
                return ref, ref, "zh"
            ref = xgat(j, xat(name[2]), other if recv else pair)
            return ref, ref, "zh"
        right = kind[0] == "R"
        link = "xp" if right else "xm"
        step = (-1 if right else 1) if recv else 0
        if modes[j] == "b" or (modes[j] == "c" and kind[1] == "1"):
            parts = (pair, other)
        else:
            parts = (own, krow(c, zl_peer, 1), krow(c, 3 - zl_peer, 1))
        if kind[1] == "3":
            at = (4 * c + 3 - zl_peer) * s + (0 if right else s // 2)
            ref = xgat(j, xat(step + (-1 if right else 1)), pl.ds(pl.multiple_of(at, 16), s // 2))
            return ref, ref, link
        if kind[1] == "1":
            ref = xgat(j, xat(step), parts[name[2]])
            direct = modes[j] in "am" and name[2] == 0 and not recv
            return (xin(j, nu) if direct else ref), ref, link
        ref = xgat(j, xat(step + (-1 if right else 1)), parts[0 if right else 1])
        return ref, ref, link

    index = {n: k for k, n in enumerate(names)}

    def remote(name, recv=False):
        src, dst, link = ends(name, recv)
        return pltpu.make_async_remote_copy(
            src_ref=src, dst_ref=dst, send_sem=ssem.at[index[name]], recv_sem=rsem.at[index[name]],
            device_id=dev[link], device_id_type=MESH)

    def stage_in(j):
        dst = xgat(j, x, krow(c, z, 1)) if j >= near else xs.at[j, :, lane(j)]
        return pltpu.make_async_copy(xin(j, nu), dst, lsem.at[j])

    def stage_out(j):
        return pltpu.make_async_copy(xs.at[j, :, lane(j)], xgat(j, x, krow(c, z, 1)), lsem.at[chunks + j])

    def a_in():
        return pltpu.make_async_copy(a_ref, av.at[y, yrow(pi)], lsem.at[2 * chunks])

    def load(task):
        j, axis, e = tasks[task]
        slot = task % SLOTS
        block = yat(e) if axis == "y" else xat(e)
        return pltpu.make_async_copy(xgat(j, block, pl.ds(0, kb)), xv.at[slot, :, lane(j)], vsem.at[slot])

    barrier = pltpu.get_barrier_semaphore()
    for peer in dev.values():
        pl.semaphore_signal(barrier, inc=1, device_id=peer, device_id_type=MESH)
    for j in range(chunks):
        stage_in(j).start()
    a_in().start()
    pl.semaphore_wait(barrier, len(dev))

    staged = [False]

    def finish_stage():
        for j in range(near):
            stage_in(j).wait()
            stage_out(j).start()
        staged[0] = True

    received = set()
    parts = [0] * chunks
    for op, what in prog:
        if op == "start":
            remote(what).start()
        elif op == "load":
            if tasks[what][0] < near:
                load(what).start()
        elif op == "wait":
            if not staged[0]:
                finish_stage()
            if what[0] == "S":
                (stage_in if what[1] >= near else stage_out)(what[1]).wait()
            elif what[0] == "AS":
                a_in().wait()
            else:
                remote(what, True).wait_recv()
                received.add(what)
        else:
            j, axis, e = tasks[what]
            slot = what % SLOTS
            wide = lane(j)
            if j < near:
                load(what).wait()
            if parts[j] == 0:
                acc[j, :, wide] = jnp.zeros((2 * s, layout[j][2]), jnp.float32)
            block = yat(e) if axis == "y" else xat(e)

            def rhs(lanes, slot=slot, block=block, j=j, wide=wide):
                return xt[j - near, block, lanes, :] if j >= near else xv[slot, lanes, wide]

            def step(k, carry, rhs=rhs, block=block, j=j, wide=wide):
                lanes = pl.ds(pl.multiple_of(k * kk, 128), kk)
                acc[j, :, wide] += jnp.dot(av[block, :, lanes], rhs(lanes), preferred_element_type=jnp.float32)
                return carry

            lax.fori_loop(0, kb // kk, step, 0)
            parts[j] += 1
            if parts[j] == 4:
                yv[j, :, wide] = acc[j, yrow(1 - pi), wide].astype(yv.dtype)
                y_ref[layout[j][0], :, cols(j, nu)] = acc[j, yrow(pi), wide].astype(y_ref.dtype)

    for name in names:
        if name not in received:
            remote(name, True).wait_recv()
    for name in names:
        remote(name).wait_send()


def solution(mesh):
    def local(a, x):
        rhs, s, xc = x.shape
        kb = a.shape[1]
        half = xc // 2
        width = 256 if half % 256 == 0 else 128
        layout = [(r, at, width) for r in range(rhs) for at in range(0, half, width)]
        if width == 256:
            split = layout[-2:]
            layout = layout[:-2] + [(r, at + more, 128) for r, at, _ in split for more in (0, 128)]
        chunks = len(layout)
        modes = (MODES * chunks)[:chunks]
        kk = 1024 if kb % 1024 == 0 else 256
        units = [2 * s * w for _, _, w in layout]
        prog, tasks, names, _ = make_plan(units, modes, 2 * s * kb // A_PIECES, BLOCK_US)
        dims = (layout, s, kb, half, kk)
        any_spec = pl.BlockSpec(memory_space=pl.ANY)
        y, _ = pl.pallas_call(
            functools.partial(body, prog, tasks, names, modes, dims),
            out_shape=(pltpu.VMEM(x.shape, x.dtype), jax.ShapeDtypeStruct((chunks, 4, kb, width), x.dtype)),
            in_specs=[any_spec, any_spec],
            out_specs=(pl.BlockSpec(memory_space=pltpu.VMEM), any_spec),
            scratch_shapes=[
                pltpu.VMEM((4, 2 * s, kb), a.dtype),
                pltpu.VMEM((SLOTS, kb, width), x.dtype),
                pltpu.VMEM((NEAR, 4, kb, layout[-1][2]), x.dtype),
                pltpu.VMEM((chunks, s, width), x.dtype),
                pltpu.VMEM((chunks, s, width), x.dtype),
                pltpu.VMEM((chunks, 2 * s, width), jnp.float32),
                pltpu.SemaphoreType.DMA((len(names),)),
                pltpu.SemaphoreType.DMA((len(names),)),
                pltpu.SemaphoreType.DMA((2 * chunks + 1,)),
                pltpu.SemaphoreType.DMA((SLOTS,)),
            ],
            compiler_params=pltpu.CompilerParams(collective_id=0, has_side_effects=True, vmem_limit_bytes=54 * 1024 * 1024),
        )(a, x)
        return y

    spec_a = P(("row", "depth"), "col")
    spec_x = P(None, ("row", "depth"), "col")
    return jax.shard_map(local, mesh=mesh, in_specs=(spec_a, spec_x), out_specs=spec_x, check_vma=False)
```
